256 devices in a mesh: fsdp: 16 (over z, core), tp: 16 (over x, y).
Axes of the slice: x: 4, y: 4, z: 8, core: 2. Of those that a mesh axis runs over, the one named last changes fastest.
Arguments:
- grad: bfloat16 [3, 5120, 27648], P(None, 'fsdp', 'tp'), may hold values from -50 to 50
- momentum: bfloat16 [3, 5120, 27648], P(None, 'fsdp', 'tp'), may hold values from -50 to 50
- basis: bfloat16 [27648, 3, 256], P(('tp', 'fsdp')), may hold values from -0.0390625 to 0.0390625
Outputs:
- momentum_next: bfloat16 [3, 5120, 27648], P(None, 'fsdp', 'tp')
- basis_next: bfloat16 [27648, 3, 256], P(('tp', 'fsdp'))
- update: bfloat16 [3, 5120, 27648], P(None, 'fsdp', 'tp')
The draws below stay inside these ranges and needn't reach their ends.
All inputs are finite; a program needn't handle non-finite values.
Results may differ from the reference program's by a relative error of at most 0.0078.
Values may be sent and summed in bfloat16 or wider, within the bound.
No kernel may reach another device: no remote copies, remote signals or barrier semaphores. Data moves between devices by JAX's collectives and lax.ppermute only.
A program may use at most 128 MiB of HBM per device.

```python
import math
import jax
import jax.numpy as jnp
from jax import lax

D = 5120
FF = 27648
RANK = 256
LAYER_COUNT = 3


def scaled_field(key):
    first, second, third = jax.random.split(key, 3)
    position = jnp.arange(FF, dtype=jnp.float32).reshape(1, 1, FF) / (FF - 1)
    base = jnp.clip(jax.random.normal(first, (LAYER_COUNT, D, FF), jnp.float32), -5.0, 5.0)
    row_scale = jnp.exp(jax.random.uniform(second, (LAYER_COUNT, D, 1), jnp.float32, -0.8, 0.8))
    col_scale = jnp.exp(jax.random.uniform(third, (LAYER_COUNT, 1, FF), jnp.float32, -0.8, 0.8))
    ramp = 1.0 + position
    return base * row_scale * col_scale * ramp


def draw_grad(key, part):
    return scaled_field(jax.random.fold_in(key, 11)).astype(jnp.bfloat16)


def draw_momentum(key, part):
    return scaled_field(jax.random.fold_in(key, 23)).astype(jnp.bfloat16)


def draw_basis(key, part):
    first, second = jax.random.split(jax.random.fold_in(key, 37))
    common = jnp.clip(jax.random.normal(first, (FF, LAYER_COUNT, 1), jnp.float32), -3.5, 3.5)
    single = jnp.clip(jax.random.normal(second, (FF, LAYER_COUNT, RANK), jnp.float32), -3.5, 3.5)
    mixed = 0.70710677 * common + 0.70710677 * single
    return (mixed / 128.0).astype(jnp.bfloat16)


def setup_inputs(seed: int = 0) -> dict:
    key_list = jax.random.split(jax.random.key(seed), 4)
    return {
        "grad": draw_grad(jax.random.fold_in(key_list[3], 71), 0),
        "momentum": draw_momentum(jax.random.fold_in(key_list[3], 71), 0),
        "basis": draw_basis(jax.random.fold_in(key_list[3], 71), 0),
    }


MOMENTUM_DECAY = 0.8
EPSILON = 1e-06

def reference(grad, momentum, basis):
    scale = math.sqrt(D * FF / RANK)
    hi = lax.Precision.HIGHEST
    moms = []
    bases = []
    updates = []
    for layer in range(LAYER_COUNT):
        buffer = MOMENTUM_DECAY * momentum[layer].astype(jnp.float32) + grad[layer].astype(jnp.float32)
        momentum_buffer16 = buffer.astype(jnp.bfloat16)
        power_output = jnp.dot(momentum_buffer16.astype(jnp.float32), basis[:, layer, :].astype(jnp.float32), preferred_element_type=jnp.float32)
        gram = jnp.dot(power_output.T, power_output, precision=hi)
        lower = jnp.linalg.cholesky(gram)
        inverse_matrix = jax.scipy.linalg.solve_triangular(lower, jnp.eye(RANK, dtype=jnp.float32), lower=True)
        ortho = jnp.dot(power_output, inverse_matrix.T, precision=hi).astype(jnp.bfloat16)
        project = jnp.dot(momentum_buffer16.T.astype(jnp.float32), ortho.astype(jnp.float32), preferred_element_type=jnp.float32)
        colsq = lax.optimization_barrier(jnp.sum(project * project, axis=0))
        basis_next = (project * lax.rsqrt(colsq + EPSILON)).astype(jnp.bfloat16)
        project16 = project.astype(jnp.bfloat16)
        feedback = jnp.dot(ortho.astype(jnp.float32), project16.T.astype(jnp.float32), preferred_element_type=jnp.float32)
        moms.append((buffer - (1.0 - MOMENTUM_DECAY) * feedback).astype(jnp.bfloat16))
        bases.append(basis_next)
        updates.append((scale * jnp.dot(ortho.astype(jnp.float32), basis_next.T.astype(jnp.float32), preferred_element_type=jnp.float32)).astype(jnp.bfloat16))
    return (jnp.stack(moms), jnp.stack(bases, axis=1), jnp.stack(updates))
```

```python
import functools
import math

import jax
import jax.numpy as jnp
from jax import lax
from jax.experimental import pallas as pl
from jax.experimental.pallas import tpu as pltpu
from jax.sharding import Mesh
from jax.sharding import PartitionSpec as P

D = 5120
FF = 27648
RANK = 256
LAYERS = 3
Z, CORE, X, Y = "fsdp_0", "fsdp_1", "tp_0", "tp_1"
FSDP = (Z, CORE)
TP = (X, Y)
TP_FSDP = TP + FSDP
Z_SIZE = 8
TP_SIZE = 16

MOMENTUM_DECAY = 0.8
EPSILON = 1e-06


def shift(value, axis, size, by):
    return lax.ppermute(value, axis, [(i, (i + by) % size) for i in range(size)])


def swap(value, axis, size, bit):
    return lax.ppermute(value, axis, [(i, i ^ bit) for i in range(size)])


def add_all(value, *axes):
    for axis, size in axes:
        bit = 1
        while bit < size:
            value = value + swap(value, axis, size, bit)
            bit *= 2
    return value


def gather_fsdp(shard):
    layers, rows, rank = shard.shape
    z, core = lax.axis_index(Z), lax.axis_index(CORE)
    half = rank // 2
    left = {1: shift(shard, Z, Z_SIZE, 1), 2: shift(shard, Z, Z_SIZE, 2)}
    right = {1: shift(shard, Z, Z_SIZE, -1), 2: shift(shard, Z, Z_SIZE, -2)}
    left[3] = shift(left[2], Z, Z_SIZE, 1)
    right[3] = shift(right[2], Z, Z_SIZE, -1)
    far = [
        shift(left[2][:, :, :half], Z, Z_SIZE, 2),
        shift(right[2][:, :, half:], Z, Z_SIZE, -2),
    ]
    mine = jnp.zeros((Z_SIZE, layers, rows, rank), shard.dtype)
    pieces = {0: shard, 4: jnp.concatenate(far, axis=2)}
    for by in (1, 2, 3):
        pieces[-by] = left[by]
        pieces[by] = right[by]
    for by, piece in pieces.items():
        mine = lax.dynamic_update_index_in_dim(mine, piece, (z + by) % Z_SIZE, 0)
    theirs = swap(mine, CORE, 2, 1)
    first = core == 0
    both = jnp.stack([jnp.where(first, mine, theirs), jnp.where(first, theirs, mine)], axis=1)
    return both.transpose(2, 0, 1, 3, 4).reshape(layers, 2 * Z_SIZE * rows, rank)


def inverse_kernel(block, group, gram_ref, out_ref, work):
    layers, rank = gram_ref.shape[0], gram_ref.shape[1]
    hi = lax.Precision.HIGHEST
    row = lax.broadcasted_iota(jnp.int32, (block, block), 0)
    lane = lax.broadcasted_iota(jnp.int32, (block, block), 1)
    eye = (row == lane).astype(jnp.float32)
    row_id = lax.broadcasted_iota(jnp.int32, (block, 2 * block), 0)
    wide = lax.broadcasted_iota(jnp.int32, (block, rank), 1)
    wide_row = lax.broadcasted_iota(jnp.int32, (block, rank), 0)
    for step in range(rank // block):
        lo, up = step * block, (step + 1) * block
        source = gram_ref if step == 0 else work
        tops = [source[l, lo:up, :] for l in range(layers)]
        mats = [jnp.concatenate([top[:, lo:up], eye], axis=1) for top in tops]
        for first in range(0, block, group):
            cols = [
                [jnp.broadcast_to(mat[:, c : c + 1], mat.shape) for c in range(first, first + group)]
                for mat in mats
            ]
            for j in range(group):
                k = first + j
                for l in range(layers):
                    mat, col = mats[l], cols[l]
                    factor = jnp.where(row_id > k, col[j] * (1.0 / col[j][k : k + 1, :]), 0.0)
                    for later in range(j + 1, group):
                        col[later] = col[later] - factor * col[later][k : k + 1, :]
                    mats[l] = mat - factor * mat[k : k + 1, :]
        for l in range(layers):
            mat = mats[l]
            pivots = jnp.sum(jnp.where(row == lane, mat[:, :block], 0.0), axis=1, keepdims=True)
            small = mat[:, block:] * lax.rsqrt(pivots)
            inside = (wide >= lo) & (wide < up)
            unit = (wide - lo == wide_row).astype(jnp.float32)
            panel = jnp.dot(
                small,
                jnp.where(inside, unit, tops[l]),
                precision=hi,
                preferred_element_type=jnp.float32,
            )
            out_ref[l, lo:up, :] = jnp.where(wide <= wide_row + lo, panel, 0.0)
            if up < rank:
                rest = source[l, up:, :]
                place = lax.broadcasted_iota(jnp.int32, rest.shape, 1)
                rest = jnp.where((place >= lo) & (place < up), 0.0, rest)
                work[l, up:, :] = rest - lax.dot_general(
                    panel[:, up:],
                    panel,
                    (((0,), (0,)), ((), ())),
                    precision=hi,
                    preferred_element_type=jnp.float32,
                )


def inverse_factor(gram):
    return pl.pallas_call(
        functools.partial(inverse_kernel, 64, 8),
        out_shape=jax.ShapeDtypeStruct(gram.shape, jnp.float32),
        in_specs=[pl.BlockSpec(memory_space=pltpu.VMEM)],
        out_specs=pl.BlockSpec(memory_space=pltpu.VMEM),
        scratch_shapes=[pltpu.VMEM(gram.shape, jnp.float32)],
        name="inverse_factor",
    )(gram)


def cross_kernel(core_ref, buffer_ref, power_ref, mine_ref, theirs_ref, whole):
    rows = mine_ref.shape[2]
    rest = power_ref[0]
    total = None
    for _ in range(3):
        part = rest.astype(jnp.bfloat16)
        rest = rest - part.astype(jnp.float32)
        term = lax.dot_general(
            buffer_ref[0], part, (((0,), (0,)), ((), ())), preferred_element_type=jnp.float32
        )
        total = term if total is None else total + term
    for j in range(2 * Z_SIZE):
        whole[j] = total[j * rows : (j + 1) * rows, :]
    core = core_ref[0]
    for j in range(Z_SIZE):
        mine_ref[0, j] = whole[2 * j + core]
        theirs_ref[0, j] = whole[2 * j + 1 - core]


def cross(buffer16, power):
    layers, rows, cols = buffer16.shape
    rank = power.shape[2]
    part = cols // (2 * Z_SIZE)
    shape = jax.ShapeDtypeStruct((layers, Z_SIZE, part, rank), jnp.float32)
    out_spec = pl.BlockSpec((1, Z_SIZE, part, rank), lambda l, core: (l, 0, 0, 0))
    return pl.pallas_call(
        cross_kernel,
        out_shape=(shape, shape),
        grid_spec=pltpu.PrefetchScalarGridSpec(
            num_scalar_prefetch=1,
            grid=(layers,),
            in_specs=[
                pl.BlockSpec((1, rows, cols), lambda l, core: (l, 0, 0)),
                pl.BlockSpec((1, rows, rank), lambda l, core: (l, 0, 0)),
            ],
            out_specs=(out_spec, out_spec),
            scratch_shapes=[pltpu.VMEM((2 * Z_SIZE, part, rank), jnp.float32)],
        ),
        name="cross",
    )(lax.axis_index(CORE).astype(jnp.int32).reshape(1), buffer16, power)


def scatter_z(blocks):
    z = lax.axis_index(Z)
    total = lax.dynamic_index_in_dim(blocks, z, 1, keepdims=False)
    arrived = []
    for by in (4, 3, 5, 2, 6, 1, 7):
        block = lax.dynamic_index_in_dim(blocks, (z + by) % Z_SIZE, 1, keepdims=False)
        arrived.append(shift(block, Z, Z_SIZE, by))
    for block in arrived:
        total = total + block
    return total


def shards(grad, momentum, basis):
    hi = lax.Precision.HIGHEST
    scale = math.sqrt(D * FF / RANK)
    buffer = MOMENTUM_DECAY * momentum.astype(jnp.float32) + grad.astype(jnp.float32)
    buffer16 = buffer.astype(jnp.bfloat16)
    layers, rows, cols = grad.shape
    tp = lax.axis_index(TP)

    basis_block = gather_fsdp(basis.transpose(1, 0, 2))
    partial = jnp.einsum(
        "lmn,lnr->lmr", buffer16, basis_block, preferred_element_type=jnp.float32
    )
    pieces = partial.reshape(layers, TP_SIZE, rows // TP_SIZE, RANK).transpose(1, 0, 2, 3)
    pieces = lax.all_to_all(pieces, TP, 0, 0, tiled=True)
    power = lax.all_gather(pieces.sum(0), TP, axis=1)
    power = power.reshape(layers, rows, RANK)

    share = RANK // TP_SIZE
    gram = jnp.einsum("lmr,lms->lrs", power, power, precision=hi)
    gram = lax.dynamic_slice_in_dim(gram, tp * share, share, 1)
    gram = add_all(gram, (CORE, 2), (Z, Z_SIZE))

    mine, theirs = cross(buffer16, power)
    mine = mine + swap(theirs, CORE, 2, 1)
    mine, gram = lax.optimization_barrier((mine, gram))
    mixed = scatter_z(mine)

    gram = lax.all_gather(gram, TP, axis=1).reshape(layers, RANK, RANK)
    inverse = inverse_factor(gram)
    ortho = jnp.einsum("lmr,lir->lmi", power, inverse, precision=hi).astype(jnp.bfloat16)

    project = jnp.einsum("lnr,lir->lni", mixed, inverse, precision=hi)
    project16 = gather_fsdp(project.astype(jnp.bfloat16))
    colsq = add_all(
        jnp.sum(project * project, axis=1), (X, 4), (Y, 4), (CORE, 2), (Z, Z_SIZE)
    )
    norm = lax.rsqrt(colsq + EPSILON)[:, None, :]
    basis_next = (project * norm).astype(jnp.bfloat16).transpose(1, 0, 2)

    feedback = jnp.einsum("lmr,lnr->lmn", ortho, project16, preferred_element_type=jnp.float32)
    momentum_next = (buffer - (1.0 - MOMENTUM_DECAY) * feedback).astype(jnp.bfloat16)
    scaled = (ortho.astype(jnp.float32) * (scale * norm)).astype(jnp.bfloat16)
    update = jnp.einsum(
        "lmr,lnr->lmn", scaled, project16, preferred_element_type=jnp.float32
    ).astype(jnp.bfloat16)
    return (momentum_next, basis_next, update)


def solution(mesh):
    torus = Mesh(mesh.devices.reshape(8, 2, 4, 4), FSDP + TP)
    return jax.shard_map(
        shards,
        mesh=torus,
        in_specs=(P(None, FSDP, TP), P(None, FSDP, TP), P(TP_FSDP, None, None)),
        out_specs=(P(None, FSDP, TP), P(TP_FSDP, None, None), P(None, FSDP, TP)),
        check_vma=False,
    )
```

```python
import functools
import math

import jax
import jax.numpy as jnp
from jax import lax
from jax.experimental import pallas as pl
from jax.experimental.pallas import tpu as pltpu
from jax.sharding import Mesh
from jax.sharding import PartitionSpec as P

D = 5120
FF = 27648
RANK = 256
LAYERS = 3
Z, CORE, X, Y = "fsdp_0", "fsdp_1", "tp_0", "tp_1"
FSDP = (Z, CORE)
TP = (X, Y)
TP_FSDP = TP + FSDP
Z_SIZE = 8
TP_SIZE = 16

MOMENTUM_DECAY = 0.8
EPSILON = 1e-06


def shift(value, axis, size, by):
    return lax.ppermute(value, axis, [(i, (i + by) % size) for i in range(size)])


def swap(value, axis, size, bit):
    return lax.ppermute(value, axis, [(i, i ^ bit) for i in range(size)])


def place_kernel(rows, seats, here_ref, near_ref, far_ref, near2_ref, far2_ref, out_ref, square_ref, blocks):
    z, core = here_ref[0], here_ref[1]
    sources = ((near_ref, far_ref), (near2_ref, far2_ref))
    for side, (near, far) in enumerate(sources):
        owner = core if side == 0 else 1 - core
        for ref, offsets in zip((near, far), seats):
            for i, by in enumerate(offsets):
                slot = 2 * lax.rem(z + by, Z_SIZE) + owner
                blocks[slot] = ref[i, 0].astype(jnp.float32)
    squares = jnp.zeros((1, out_ref.shape[2]), jnp.float32)
    parts = []
    for j in range(2 * Z_SIZE):
        block = blocks[j][:rows, :]
        squares = squares + jnp.sum(block * block, axis=0, keepdims=True)
        parts.append(block)
    out_ref[0] = jnp.concatenate(parts, axis=0).astype(out_ref.dtype)
    square_ref[0] = squares


def position():
    return jnp.stack([lax.axis_index(Z), lax.axis_index(CORE)]).astype(jnp.int32)


def place(near, far, near2, far2, rows, seats):
    _, layers, padded, rank = near.shape

    def spec(n):
        return pl.BlockSpec((n, 1, padded, rank), lambda l, here: (0, l, 0, 0))

    total = 2 * Z_SIZE * rows
    return pl.pallas_call(
        functools.partial(place_kernel, rows, seats),
        out_shape=(
            jax.ShapeDtypeStruct((layers, total, rank), near.dtype),
            jax.ShapeDtypeStruct((layers, 1, rank), jnp.float32),
        ),
        grid_spec=pltpu.PrefetchScalarGridSpec(
            num_scalar_prefetch=1,
            grid=(layers,),
            in_specs=[spec(5), spec(3), spec(5), spec(3)],
            out_specs=(
                pl.BlockSpec((1, total, rank), lambda l, here: (l, 0, 0)),
                pl.BlockSpec((1, 1, rank), lambda l, here: (l, 0, 0)),
            ),
            scratch_shapes=[pltpu.VMEM((2 * Z_SIZE, padded, rank), jnp.float32)],
        ),
        name="place",
    )(position(), near, far, near2, far2)


def gather_fsdp(shard, rows):
    half = shard.shape[2] // 2
    left = shift(shard, Z, Z_SIZE, 1)
    right = shift(shard, Z, Z_SIZE, -1)
    left2 = shift(shard, Z, Z_SIZE, 2)
    right2 = shift(shard, Z, Z_SIZE, -2)
    left3 = shift(left2, Z, Z_SIZE, 1)
    right3 = shift(right2, Z, Z_SIZE, -1)
    far_left = shift(left2[:, :, :half], Z, Z_SIZE, 2)
    far_right = shift(right2[:, :, half:], Z, Z_SIZE, -2)
    near = jnp.stack([shard, left, right, left2, right2])
    near2 = swap(near, CORE, 2, 1)
    far = jnp.stack([left3, right3, jnp.concatenate([far_left, far_right], axis=2)])
    far2 = swap(far, CORE, 2, 1)
    return place(near, far, near2, far2, rows, ((0, 7, 1, 6, 2), (5, 3, 4)))


def inverse_kernel(block, group, gram_ref, out_ref, work):
    layers, rank = gram_ref.shape[0], gram_ref.shape[1]
    hi = lax.Precision.HIGHEST
    row = lax.broadcasted_iota(jnp.int32, (block, block), 0)
    lane = lax.broadcasted_iota(jnp.int32, (block, block), 1)
    eye = (row == lane).astype(jnp.float32)
    row_id = lax.broadcasted_iota(jnp.int32, (block, 2 * block), 0)
    wide = lax.broadcasted_iota(jnp.int32, (block, rank), 1)
    wide_row = lax.broadcasted_iota(jnp.int32, (block, rank), 0)
    for step in range(rank // block):
        lo, up = step * block, (step + 1) * block
        source = gram_ref if step == 0 else work
        tops = [source[l, lo:up, :] for l in range(layers)]
        mats = [jnp.concatenate([top[:, lo:up], eye], axis=1) for top in tops]
        for first in range(0, block, group):
            cols = [
                [jnp.broadcast_to(mat[:, c : c + 1], mat.shape) for c in range(first, first + group)]
                for mat in mats
            ]
            for j in range(group):
                k = first + j
                for l in range(layers):
                    mat, col = mats[l], cols[l]
                    factor = jnp.where(row_id > k, col[j] * (1.0 / col[j][k : k + 1, :]), 0.0)
                    for later in range(j + 1, group):
                        col[later] = col[later] - factor * col[later][k : k + 1, :]
                    mats[l] = mat - factor * mat[k : k + 1, :]
        for l in range(layers):
            mat = mats[l]
            pivots = jnp.sum(jnp.where(row == lane, mat[:, :block], 0.0), axis=1, keepdims=True)
            small = mat[:, block:] * lax.rsqrt(pivots)
            inside = (wide >= lo) & (wide < up)
            unit = (wide - lo == wide_row).astype(jnp.float32)
            panel = jnp.dot(
                small,
                jnp.where(inside, unit, tops[l]),
                precision=hi,
                preferred_element_type=jnp.float32,
            )
            out_ref[l, lo:up, :] = jnp.where(wide <= wide_row + lo, panel, 0.0)
            if up < rank:
                rest = source[l, up:, :]
                place = lax.broadcasted_iota(jnp.int32, rest.shape, 1)
                rest = jnp.where((place >= lo) & (place < up), 0.0, rest)
                work[l, up:, :] = rest - lax.dot_general(
                    panel[:, up:],
                    panel,
                    (((0,), (0,)), ((), ())),
                    precision=hi,
                    preferred_element_type=jnp.float32,
                )


def inverse_factor(gram):
    return pl.pallas_call(
        functools.partial(inverse_kernel, 64, 8),
        out_shape=jax.ShapeDtypeStruct(gram.shape, jnp.float32),
        in_specs=[pl.BlockSpec(memory_space=pltpu.VMEM)],
        out_specs=pl.BlockSpec(memory_space=pltpu.VMEM),
        scratch_shapes=[pltpu.VMEM(gram.shape, jnp.float32)],
        name="inverse_factor",
    )(gram)


def cross_kernel(part, here_ref, buffer_ref, power_ref, *refs):
    mine_ref, theirs_ref, whole = refs[-3:]
    rest = power_ref[0]
    total = None
    for _ in range(3):
        piece = rest.astype(jnp.bfloat16)
        rest = rest - piece.astype(jnp.float32)
        term = lax.dot_general(
            buffer_ref[0], piece, (((0,), (0,)), ((), ())), preferred_element_type=jnp.float32
        )
        total = term if total is None else total + term
    padding = jnp.zeros((whole.shape[1] - part, whole.shape[2]), jnp.float32)
    for j in range(2 * Z_SIZE):
        whole[j] = jnp.concatenate([total[j * part : (j + 1) * part, :], padding], axis=0)
    z, core = here_ref[0], here_ref[1]
    for by in range(Z_SIZE):
        slot = 2 * lax.rem(z + by, Z_SIZE)
        mine_ref[by, 0] = whole[slot + core]
        theirs_ref[by, 0] = whole[slot + 1 - core]


def cross(layer, buffer16, power, padded, before):
    layers, rows, cols = buffer16.shape
    rank = power.shape[2]
    part = cols // (2 * Z_SIZE)
    shape = jax.ShapeDtypeStruct((Z_SIZE, layers, padded, rank), jnp.float32)
    out_spec = pl.BlockSpec((Z_SIZE, 1, padded, rank), lambda i, here: (0, layer, 0, 0))
    extra = () if before is None else before
    return pl.pallas_call(
        functools.partial(cross_kernel, part),
        out_shape=(shape, shape),
        grid_spec=pltpu.PrefetchScalarGridSpec(
            num_scalar_prefetch=1,
            grid=(1,),
            in_specs=[
                pl.BlockSpec((1, rows, cols), lambda i, here: (layer, 0, 0)),
                pl.BlockSpec((1, rows, rank), lambda i, here: (layer, 0, 0)),
            ]
            + [pl.BlockSpec(memory_space=pl.ANY) for _ in extra],
            out_specs=(out_spec, out_spec),
            scratch_shapes=[pltpu.VMEM((2 * Z_SIZE, padded, rank), jnp.float32)],
        ),
        input_output_aliases={} if before is None else {3: 0, 4: 1},
        name="cross",
    )(position(), buffer16, power, *extra)


def scatter_near(blocks):
    half = blocks.shape[3] // 2
    left3 = shift(blocks[3], Z, Z_SIZE, 1)
    right3 = shift(blocks[5], Z, Z_SIZE, -1)
    left4 = shift(blocks[4][:, :, :half], Z, Z_SIZE, 2)
    right4 = shift(blocks[4][:, :, half:], Z, Z_SIZE, -2)
    one = shift(blocks[1], Z, Z_SIZE, 1)
    seven = shift(blocks[7], Z, Z_SIZE, -1)
    two = blocks[2] + left3
    two = jnp.concatenate([two[:, :, :half] + left4, two[:, :, half:]], axis=2)
    six = blocks[6] + right3
    six = jnp.concatenate([six[:, :, :half], six[:, :, half:] + right4], axis=2)
    return blocks[0] + one + seven, two, six


def scatter_far(total, two, six):
    return total + shift(two, Z, Z_SIZE, 2) + shift(six, Z, Z_SIZE, -2)


def total_over(value, axis, size):
    return value + shift(value, axis, size, 1) + shift(value, axis, size, -1) + shift(value, axis, size, 2)


def shards(grad, momentum, basis):
    hi = lax.Precision.HIGHEST
    scale = math.sqrt(D * FF / RANK)
    buffer = MOMENTUM_DECAY * momentum.astype(jnp.float32) + grad.astype(jnp.float32)
    buffer16 = buffer.astype(jnp.bfloat16)
    layers, rows, cols = grad.shape
    tp = lax.axis_index(TP)
    part = basis.shape[0]
    padded = -(-part // 16) * 16

    shard = jnp.pad(basis.transpose(1, 0, 2), ((0, 0), (0, padded - part), (0, 0)))
    basis_block, _ = gather_fsdp(shard, part)
    partial = jnp.einsum(
        "lmn,lnr->lmr", buffer16, basis_block, preferred_element_type=jnp.float32
    )
    pieces = partial.reshape(layers, TP_SIZE, rows // TP_SIZE, RANK).transpose(1, 0, 2, 3)
    pieces = lax.all_to_all(pieces, TP, 0, 0, tiled=True)
    power = lax.all_gather(pieces.sum(0), TP, axis=1)
    power = power.reshape(layers, rows, RANK)

    share = RANK // TP_SIZE
    gram = jnp.einsum("lmr,lms->lrs", power, power, precision=hi)
    gram = lax.dynamic_slice_in_dim(gram, tp * share, share, 1)
    blocks, right = None, power
    for layer, (axis, size, bit) in enumerate(((CORE, 2, 1), (Z, Z_SIZE, 1), (Z, Z_SIZE, 2))):
        gram, right = lax.optimization_barrier((gram, right))
        blocks = cross(layer, buffer16, right, padded, blocks)
        gram = gram + swap(gram, axis, size, bit)
    gram = gram + swap(gram, Z, Z_SIZE, 4)
    mine, theirs = blocks
    mine = mine + swap(theirs, CORE, 2, 1)
    mine, gram = lax.optimization_barrier((mine, gram))
    hops = scatter_near(mine)

    gram = lax.all_gather(gram, TP, axis=1).reshape(layers, RANK, RANK)
    gram, *hops = lax.optimization_barrier((gram, *hops))
    mixed = scatter_far(*hops)
    inverse = inverse_factor(gram)
    ortho = jnp.einsum("lmr,lir->lmi", power, inverse, precision=hi).astype(jnp.bfloat16)

    project = jnp.einsum("lnr,lir->lni", mixed, inverse, precision=hi)
    project16, colsq = gather_fsdp(project.astype(jnp.bfloat16), part)
    colsq = total_over(total_over(colsq, X, 4), Y, 4)
    norm = lax.rsqrt(colsq + EPSILON)
    basis_next = (project[:, :part] * norm).astype(jnp.bfloat16).transpose(1, 0, 2)

    feedback = jnp.einsum("lmr,lnr->lmn", ortho, project16, preferred_element_type=jnp.float32)
    momentum_next = (buffer - (1.0 - MOMENTUM_DECAY) * feedback).astype(jnp.bfloat16)
    scaled = (ortho.astype(jnp.float32) * (scale * norm)).astype(jnp.bfloat16)
    update = jnp.einsum(
        "lmr,lnr->lmn", scaled, project16, preferred_element_type=jnp.float32
    ).astype(jnp.bfloat16)
    return (momentum_next, basis_next, update)


def solution(mesh):
    torus = Mesh(mesh.devices.reshape(8, 2, 4, 4), FSDP + TP)
    return jax.shard_map(
        shards,
        mesh=torus,
        in_specs=(P(None, FSDP, TP), P(None, FSDP, TP), P(TP_FSDP, None, None)),
        out_specs=(P(None, FSDP, TP), P(TP_FSDP, None, None), P(None, FSDP, TP)),
        check_vma=False,
    )
```

```python
import functools
import math

import jax
import jax.numpy as jnp
from jax import lax
from jax.experimental import pallas as pl
from jax.experimental.pallas import tpu as pltpu
from jax.sharding import Mesh
from jax.sharding import PartitionSpec as P

D = 5120
FF = 27648
RANK = 256
LAYERS = 3
Z, CORE, X, Y = "fsdp_0", "fsdp_1", "tp_0", "tp_1"
FSDP = (Z, CORE)
TP = (X, Y)
TP_FSDP = TP + FSDP
Z_SIZE = 8
TP_SIZE = 16

MOMENTUM_DECAY = 0.8
EPSILON = 1e-06


def shift(value, axis, size, by):
    return lax.ppermute(value, axis, [(i, (i + by) % size) for i in range(size)])


def swap(value, axis, size, bit):
    return lax.ppermute(value, axis, [(i, i ^ bit) for i in range(size)])


def turn(value, by):
    pairs = []
    for z in range(Z_SIZE):
        pairs.append((2 * z, 2 * ((z + by) % Z_SIZE)))
        pairs.append((2 * z + 1, 2 * ((z - by) % Z_SIZE) + 1))
    return lax.ppermute(value, FSDP, pairs)


def position():
    return jnp.stack([lax.axis_index(Z), lax.axis_index(CORE)]).astype(jnp.int32)


def gather_fsdp(pair, busy=None):
    one = turn(pair, 1)
    two = turn(pair, 2)
    if busy is not None:
        two, busy = lax.optimization_barrier((two, busy))
    three = turn(two, 1)
    four = turn(two[0], 2)
    near = jnp.concatenate([one, two])
    near2 = swap(near, CORE, 2, 1)
    far = jnp.concatenate([three, four[None]])
    far2 = swap(far, CORE, 2, 1)
    return (pair, near, near2, far, far2), busy


def join(rows, here_ref, refs, layer, blocks):
    z, core = here_ref[0], here_ref[1]
    ahead = 2 * core - 1
    for ref, first, way, owner in zip(
        refs, (0, 1, 1, 3, 3), (0, ahead, -ahead, ahead, -ahead), (core, core, 1 - core, core, 1 - core)
    ):
        for i in range(ref.shape[0]):
            place = lax.rem(z + (first + i // 2) * way + Z_SIZE, Z_SIZE)
            whose = owner if i % 2 == 0 else 1 - owner
            blocks[2 * place + whose] = ref[i, layer].astype(jnp.float32)
    return jnp.concatenate([blocks[j][:rows, :] for j in range(2 * Z_SIZE)], axis=0)


def place_kernel(rows, here_ref, *refs):
    out_ref, square_ref, blocks = refs[-3:]
    whole = join(rows, here_ref, refs[:-3], 0, blocks)
    out_ref[0] = whole.astype(out_ref.dtype)
    square_ref[0] = jnp.sum(whole * whole, axis=0, keepdims=True)


def power_kernel(rows, here_ref, buffer_ref, *refs):
    out_ref, blocks = refs[-2:]
    whole = join(rows, here_ref, refs[:-2], 0, blocks).astype(jnp.bfloat16)
    product = jnp.dot(buffer_ref[0], whole, preferred_element_type=jnp.float32)
    share = out_ref.shape[2]
    for t in range(out_ref.shape[0]):
        out_ref[t, 0] = product[t * share : (t + 1) * share, :]


def piece_specs(pieces):
    return [
        pl.BlockSpec((p.shape[0], 1) + p.shape[2:], lambda l, here: (0, l, 0, 0)) for p in pieces
    ]


def place(pieces, rows):
    _, layers, padded, rank = pieces[0].shape
    total = 2 * Z_SIZE * rows
    return pl.pallas_call(
        functools.partial(place_kernel, rows),
        out_shape=(
            jax.ShapeDtypeStruct((layers, total, rank), pieces[0].dtype),
            jax.ShapeDtypeStruct((layers, 1, rank), jnp.float32),
        ),
        grid_spec=pltpu.PrefetchScalarGridSpec(
            num_scalar_prefetch=1,
            grid=(layers,),
            in_specs=piece_specs(pieces),
            out_specs=(
                pl.BlockSpec((1, total, rank), lambda l, here: (l, 0, 0)),
                pl.BlockSpec((1, 1, rank), lambda l, here: (l, 0, 0)),
            ),
            scratch_shapes=[pltpu.VMEM((2 * Z_SIZE, padded, rank), jnp.float32)],
        ),
        name="place",
    )(position(), *pieces)


def power_step(buffer16, pieces, rows):
    layers, height, cols = buffer16.shape
    padded, rank = pieces[0].shape[2:]
    share = height // TP_SIZE
    return pl.pallas_call(
        functools.partial(power_kernel, rows),
        out_shape=jax.ShapeDtypeStruct((TP_SIZE, layers, share, rank), jnp.float32),
        grid_spec=pltpu.PrefetchScalarGridSpec(
            num_scalar_prefetch=1,
            grid=(layers,),
            in_specs=[pl.BlockSpec((1, height, cols), lambda l, here: (l, 0, 0))]
            + piece_specs(pieces),
            out_specs=pl.BlockSpec((TP_SIZE, 1, share, rank), lambda l, here: (0, l, 0, 0)),
            scratch_shapes=[pltpu.VMEM((2 * Z_SIZE, padded, rank), jnp.float32)],
        ),
        name="power",
    )(position(), buffer16, *pieces)


def inverse_kernel(block, group, gram_ref, out_ref, work):
    layers, rank = gram_ref.shape[0], gram_ref.shape[1]
    hi = lax.Precision.HIGHEST
    row = lax.broadcasted_iota(jnp.int32, (block, block), 0)
    lane = lax.broadcasted_iota(jnp.int32, (block, block), 1)
    eye = (row == lane).astype(jnp.float32)
    row_id = lax.broadcasted_iota(jnp.int32, (block, 2 * block), 0)
    wide = lax.broadcasted_iota(jnp.int32, (block, rank), 1)
    wide_row = lax.broadcasted_iota(jnp.int32, (block, rank), 0)
    place = lax.broadcasted_iota(jnp.int32, (rank, rank), 1)
    work[...] = gram_ref[...]

    def eliminate(step, _):
        lo = pl.multiple_of(step * block, block)
        tops = [work[l, pl.ds(lo, block), :] for l in range(layers)]
        diag = [pltpu.roll(top, rank - lo, 1)[:, :block] for top in tops]
        tails = [jnp.concatenate([d, eye], axis=1) for d in diag]
        ready = [[] for _ in range(layers)]
        for first in range(0, block, group):
            cols = [
                [jnp.broadcast_to(tail[:, c : c + 1], tail.shape) for c in range(first, first + group)]
                for tail in tails
            ]
            below = row_id[first:, :]
            for j in range(group):
                for l in range(layers):
                    tail, col = tails[l], cols[l]
                    factor = jnp.where(below > first + j, col[j] * (1.0 / col[j][j : j + 1, :]), 0.0)
                    for later in range(j + 1, group):
                        col[later] = col[later] - factor * col[later][j : j + 1, :]
                    tails[l] = tail - factor * tail[j : j + 1, :]
            for l in range(layers):
                ready[l].append(tails[l][:group, :])
                tails[l] = tails[l][group:, :]
        mats = [jnp.concatenate(parts, axis=0) for parts in ready]
        inside = (wide >= lo) & (wide < lo + block)
        unit = (wide - lo == wide_row).astype(jnp.float32)
        panels = []
        own = (place >= lo) & (place < lo + block)
        for l in range(layers):
            mat = mats[l]
            pivots = jnp.sum(jnp.where(row == lane, mat[:, :block], 0.0), axis=1, keepdims=True)
            small = mat[:, block:] * lax.rsqrt(pivots)
            panel = jnp.dot(small, jnp.where(inside, unit, tops[l]), precision=hi, preferred_element_type=jnp.float32)
            out_ref[l, pl.ds(lo, block), :] = jnp.where(wide <= wide_row + lo, panel, 0.0)
            panels.append(panel)

        @pl.when(step < rank // block - 1)
        def _():
            for l in range(layers):
                work[l] = jnp.where(own, 0.0, work[l]) - lax.dot_general(
                    panels[l], panels[l], (((0,), (0,)), ((), ())), precision=hi, preferred_element_type=jnp.float32)

        return 0

    lax.fori_loop(0, rank // block, eliminate, 0)

def inverse_factor(gram):
    return pl.pallas_call(
        functools.partial(inverse_kernel, 32, 8),
        out_shape=jax.ShapeDtypeStruct(gram.shape, jnp.float32),
        in_specs=[pl.BlockSpec(memory_space=pltpu.VMEM)],
        out_specs=pl.BlockSpec(memory_space=pltpu.VMEM),
        scratch_shapes=[pltpu.VMEM(gram.shape, jnp.float32)],
        name="inverse_factor",
    )(gram)


def cross_kernel(part, here_ref, buffer_ref, power_ref, mine_ref, theirs_ref, whole):
    rest = power_ref[0]
    total = None
    for _ in range(3):
        piece = rest.astype(jnp.bfloat16)
        rest = rest - piece.astype(jnp.float32)
        term = lax.dot_general(
            buffer_ref[0], piece, (((0,), (0,)), ((), ())), preferred_element_type=jnp.float32
        )
        total = term if total is None else total + term
    padding = jnp.zeros((whole.shape[1] - part, whole.shape[2]), jnp.float32)
    for j in range(2 * Z_SIZE):
        whole[j] = jnp.concatenate([total[j * part : (j + 1) * part, :], padding], axis=0)
    z, core = here_ref[0], here_ref[1]
    for ref, owner in ((mine_ref, core), (theirs_ref, 1 - core)):
        for i in range(Z_SIZE):
            by = (1, 1, 2, 2, 3, 3, 4, 0)[i]
            place = lax.rem(z + by * (1 - 2 * owner) + Z_SIZE, Z_SIZE)
            whose = 1 - owner if i in (1, 3, 5) else owner
            ref[i, 0] = whole[2 * place + whose]


def cross(buffer16, power, padded):
    layers, rows, cols = buffer16.shape
    rank = power.shape[2]
    shape = jax.ShapeDtypeStruct((Z_SIZE, layers, padded, rank), jnp.float32)
    out_spec = pl.BlockSpec((Z_SIZE, 1, padded, rank), lambda l, here: (0, l, 0, 0))
    return pl.pallas_call(
        functools.partial(cross_kernel, cols // (2 * Z_SIZE)),
        out_shape=(shape, shape),
        grid_spec=pltpu.PrefetchScalarGridSpec(
            num_scalar_prefetch=1,
            grid=(layers,),
            in_specs=[
                pl.BlockSpec((1, rows, cols), lambda l, here: (l, 0, 0)),
                pl.BlockSpec((1, rows, rank), lambda l, here: (l, 0, 0)),
            ],
            out_specs=(out_spec, out_spec),
            scratch_shapes=[pltpu.VMEM((2 * Z_SIZE, padded, rank), jnp.float32)],
        ),
        name="cross",
    )(position(), buffer16, power)


def scatter_near(blocks):
    three, four, one = lax.optimization_barrier((blocks[4:6], blocks[6], blocks[0:2]))
    three, four, one = turn(three, 1), turn(four, 2), turn(one, 1)
    three, four, one = lax.optimization_barrier((three, four, one))
    two = jnp.stack([blocks[2] + three[0] + four, blocks[3] + three[1]])
    return blocks[7], one, two


def scatter_end(own, one, far):
    total = one + far
    total = jnp.stack([own + total[0], total[1]])
    other = swap(total, CORE, 2, 1)
    return jnp.stack([total[0] + other[1], total[1] + other[0]])


def total_over(value, axis, size):
    return value + shift(value, axis, size, 1) + shift(value, axis, size, -1) + shift(value, axis, size, 2)


def shards(grad, momentum, basis):
    hi = lax.Precision.HIGHEST
    scale = math.sqrt(D * FF / RANK)
    buffer = MOMENTUM_DECAY * momentum.astype(jnp.float32) + grad.astype(jnp.float32)
    buffer16 = buffer.astype(jnp.bfloat16)
    layers, rows, cols = grad.shape
    tp = lax.axis_index(TP)
    part = basis.shape[0]
    padded = -(-part // 16) * 16

    shard = jnp.pad(basis.transpose(1, 0, 2), ((0, 0), (0, padded - part), (0, 0)))
    pair = jnp.stack([shard, swap(shard, CORE, 2, 1)])
    pieces, buffer16 = gather_fsdp(pair, buffer16)
    partial = lax.all_to_all(power_step(buffer16, pieces, part), TP, 0, 0, tiled=True)
    power = lax.all_gather(partial.sum(0), TP, axis=1).reshape(layers, rows, RANK)

    share = RANK // TP_SIZE
    gram = jnp.einsum("lmr,lms->lrs", power, power, precision=hi)
    gram = lax.dynamic_slice_in_dim(gram, tp * share, share, 1)
    gram, right = lax.optimization_barrier((gram, power))
    mine, theirs = cross(buffer16, right, padded)
    gram = gram + swap(gram, CORE, 2, 1)
    for bit in (1, 2, 4):
        gram = gram + swap(gram, Z, Z_SIZE, bit)
    mine = mine + swap(theirs, CORE, 2, 1)
    mine, gram = lax.optimization_barrier((mine, gram))
    hops = scatter_near(mine)

    gram = lax.all_gather(gram, TP, axis=1).reshape(layers, RANK, RANK)
    gram, *hops = lax.optimization_barrier((gram, *hops))
    own, one, two = hops
    far, inverse = lax.optimization_barrier((turn(two, 2), inverse_factor(gram)))
    mixed = scatter_end(own, one, far)
    ortho = jnp.einsum("lmr,lir->lmi", power, inverse, precision=hi).astype(jnp.bfloat16)

    project = jnp.einsum("clnr,lir->clni", mixed, inverse, precision=hi)
    pieces, _ = gather_fsdp(project.astype(jnp.bfloat16))
    project16, colsq = place(pieces, part)
    colsq = total_over(total_over(colsq, X, 4), Y, 4)
    norm = lax.rsqrt(colsq + EPSILON)
    basis_next = (project[0, :, :part] * norm).astype(jnp.bfloat16).transpose(1, 0, 2)

    feedback = jnp.einsum("lmr,lnr->lmn", ortho, project16, preferred_element_type=jnp.float32)
    momentum_next = (buffer - (1.0 - MOMENTUM_DECAY) * feedback).astype(jnp.bfloat16)
    scaled = (ortho.astype(jnp.float32) * (scale * norm)).astype(jnp.bfloat16)
    update = jnp.einsum(
        "lmr,lnr->lmn", scaled, project16, preferred_element_type=jnp.float32
    ).astype(jnp.bfloat16)
    return (momentum_next, basis_next, update)


def solution(mesh):
    torus = Mesh(mesh.devices.reshape(8, 2, 4, 4), FSDP + TP)
    return jax.shard_map(
        shards,
        mesh=torus,
        in_specs=(P(None, FSDP, TP), P(None, FSDP, TP), P(TP_FSDP, None, None)),
        out_specs=(P(None, FSDP, TP), P(TP_FSDP, None, None), P(None, FSDP, TP)),
        check_vma=False,
    )
```

```python
import functools
import math

import jax
import jax.numpy as jnp
from jax import lax
from jax.experimental import pallas as pl
from jax.experimental.pallas import tpu as pltpu
from jax.sharding import Mesh
from jax.sharding import PartitionSpec as P

D = 5120
FF = 27648
RANK = 256
LAYERS = 3
Z, CORE, X, Y = "fsdp_0", "fsdp_1", "tp_0", "tp_1"
FSDP = (Z, CORE)
TP = (X, Y)
TP_FSDP = TP + FSDP
Z_SIZE = 8
TP_SIZE = 16

MOMENTUM_DECAY = 0.8
EPSILON = 1e-06


def shift(value, axis, size, by):
    return lax.ppermute(value, axis, [(i, (i + by) % size) for i in range(size)])


def swap(value, axis, size, bit):
    return lax.ppermute(value, axis, [(i, i ^ bit) for i in range(size)])


def turn(value, by):
    pairs = []
    for z in range(Z_SIZE):
        pairs.append((2 * z, 2 * ((z + by) % Z_SIZE)))
        pairs.append((2 * z + 1, 2 * ((z - by) % Z_SIZE) + 1))
    return lax.ppermute(value, FSDP, pairs)


def position():
    return jnp.stack([lax.axis_index(Z), lax.axis_index(CORE)]).astype(jnp.int32)


def crossing(value):
    pairs = []
    for z in range(Z_SIZE):
        pairs.append((2 * z, 2 * ((z + 1) % Z_SIZE) + 1))
        pairs.append((2 * z + 1, 2 * ((z - 1) % Z_SIZE)))
    return lax.ppermute(value, FSDP, pairs)


def add_one(value):
    return value + turn(value, 1)


def add_two(value):
    return value + turn(value, 2)


def add_crossing(value):
    return value + crossing(value)


def add_square(axis, value):
    return value + shift(value, axis, 4, 1) + shift(value, axis, 4, -1) + shift(value, axis, 4, 2)


def gather_fsdp(pair, side, stages):
    stages = list(stages)

    def hop(value, side):
        moved = turn(value, 1)
        if stages:
            moved, side = lax.optimization_barrier((moved, stages.pop(0)(side)))
        return moved, side

    one, side = hop(pair, side)
    two, side = hop(one, side)
    near = jnp.concatenate([one, two])
    near2 = swap(near, CORE, 2, 1)
    three, side = hop(two, side)
    four, side = hop(three[0], side)
    far = jnp.concatenate([three, four[None]])
    far2 = swap(far, CORE, 2, 1)
    for stage in stages:
        side = stage(side)
    return (pair, near, near2, far, far2), side


def join(rows, here_ref, refs, layer, blocks):
    z, core = here_ref[0], here_ref[1]
    ahead = 2 * core - 1
    for ref, first, way, owner in zip(
        refs, (0, 1, 1, 3, 3), (0, ahead, -ahead, ahead, -ahead), (core, core, 1 - core, core, 1 - core)
    ):
        for i in range(ref.shape[0]):
            place = lax.rem(z + (first + i // 2) * way + Z_SIZE, Z_SIZE)
            whose = owner if i % 2 == 0 else 1 - owner
            blocks[2 * place + whose] = ref[i, layer].astype(jnp.float32)
    return jnp.concatenate([blocks[j][:rows, :] for j in range(2 * Z_SIZE)], axis=0)


def finish_kernel(rows, scale, here_ref, grad_ref, momentum_ref, ortho_ref, norm_ref, *refs):
    momentum_next_ref, update_ref, blocks = refs[-3:]
    whole = join(rows, here_ref, refs[:-3], 0, blocks).astype(jnp.bfloat16)
    ortho = ortho_ref[0]
    scaled = (ortho.astype(jnp.float32) * (scale * norm_ref[0])).astype(jnp.bfloat16)
    last = (((1,), (1,)), ((), ()))
    feedback = lax.dot_general(ortho, whole, last, preferred_element_type=jnp.float32)
    buffer = MOMENTUM_DECAY * momentum_ref[0].astype(jnp.float32) + grad_ref[0].astype(jnp.float32)
    momentum_next_ref[0] = (buffer - (1.0 - MOMENTUM_DECAY) * feedback).astype(jnp.bfloat16)
    update = lax.dot_general(scaled, whole, last, preferred_element_type=jnp.float32)
    update_ref[0] = update.astype(jnp.bfloat16)


def power_kernel(rows, here_ref, buffer_ref, *refs):
    out_ref, blocks = refs[-2:]
    whole = join(rows, here_ref, refs[:-2], 0, blocks).astype(jnp.bfloat16)
    product = jnp.dot(buffer_ref[0], whole, preferred_element_type=jnp.float32)
    share = out_ref.shape[2]
    for t in range(out_ref.shape[0]):
        out_ref[t, 0] = product[t * share : (t + 1) * share, :]


def piece_specs(pieces):
    return [
        pl.BlockSpec((p.shape[0], 1) + p.shape[2:], lambda l, here: (0, l, 0, 0)) for p in pieces
    ]


def finish(grad, momentum, ortho, norm, pieces, rows, scale):
    layers, height, cols = grad.shape
    padded, rank = pieces[0].shape[2:]
    shape = jax.ShapeDtypeStruct(grad.shape, grad.dtype)

    def spec(m, n):
        return pl.BlockSpec((1, m, n), lambda l, here: (l, 0, 0))

    return pl.pallas_call(
        functools.partial(finish_kernel, rows, scale),
        out_shape=(shape, shape),
        grid_spec=pltpu.PrefetchScalarGridSpec(
            num_scalar_prefetch=1,
            grid=(layers,),
            in_specs=[spec(height, cols), spec(height, cols), spec(height, rank), spec(1, rank)]
            + piece_specs(pieces),
            out_specs=(spec(height, cols), spec(height, cols)),
            scratch_shapes=[pltpu.VMEM((2 * Z_SIZE, padded, rank), jnp.float32)],
        ),
        name="finish",
    )(position(), grad, momentum, ortho, norm, *pieces)


def power_step(buffer16, pieces, rows):
    layers, height, cols = buffer16.shape
    padded, rank = pieces[0].shape[2:]
    share = height // TP_SIZE
    return pl.pallas_call(
        functools.partial(power_kernel, rows),
        out_shape=jax.ShapeDtypeStruct((TP_SIZE, layers, share, rank), jnp.float32),
        grid_spec=pltpu.PrefetchScalarGridSpec(
            num_scalar_prefetch=1,
            grid=(layers,),
            in_specs=[pl.BlockSpec((1, height, cols), lambda l, here: (l, 0, 0))]
            + piece_specs(pieces),
            out_specs=pl.BlockSpec((TP_SIZE, 1, share, rank), lambda l, here: (0, l, 0, 0)),
            scratch_shapes=[pltpu.VMEM((2 * Z_SIZE, padded, rank), jnp.float32)],
        ),
        name="power",
    )(position(), buffer16, *pieces)


def inverse_kernel(block, group, gram_ref, out_ref, work):
    layers, rank = gram_ref.shape[0], gram_ref.shape[1]
    hi = lax.Precision.HIGHEST
    row = lax.broadcasted_iota(jnp.int32, (block, block), 0)
    lane = lax.broadcasted_iota(jnp.int32, (block, block), 1)
    eye = (row == lane).astype(jnp.float32)
    row_id = lax.broadcasted_iota(jnp.int32, (block, 2 * block), 0)
    wide = lax.broadcasted_iota(jnp.int32, (block, rank), 1)
    wide_row = lax.broadcasted_iota(jnp.int32, (block, rank), 0)
    place = lax.broadcasted_iota(jnp.int32, (rank, rank), 1)
    work[...] = gram_ref[...]

    def eliminate(step, _):
        lo = pl.multiple_of(step * block, block)
        tops = [work[l, pl.ds(lo, block), :] for l in range(layers)]
        diag = [pltpu.roll(top, rank - lo, 1)[:, :block] for top in tops]
        tails = [jnp.concatenate([d, eye], axis=1) for d in diag]
        ready = [[] for _ in range(layers)]
        for first in range(0, block, group):
            cols = [
                [jnp.broadcast_to(tail[:, c : c + 1], tail.shape) for c in range(first, first + group)]
                for tail in tails
            ]
            below = row_id[first:, :]
            for j in range(group):
                for l in range(layers):
                    tail, col = tails[l], cols[l]
                    factor = jnp.where(below > first + j, col[j] * (1.0 / col[j][j : j + 1, :]), 0.0)
                    for later in range(j + 1, group):
                        col[later] = col[later] - factor * col[later][j : j + 1, :]
                    tails[l] = tail - factor * tail[j : j + 1, :]
            for l in range(layers):
                ready[l].append(tails[l][:group, :])
                tails[l] = tails[l][group:, :]
        mats = [jnp.concatenate(parts, axis=0) for parts in ready]
        inside = (wide >= lo) & (wide < lo + block)
        unit = (wide - lo == wide_row).astype(jnp.float32)
        panels = []
        own = (place >= lo) & (place < lo + block)
        for l in range(layers):
            mat = mats[l]
            pivots = jnp.sum(jnp.where(row == lane, mat[:, :block], 0.0), axis=1, keepdims=True)
            small = mat[:, block:] * lax.rsqrt(pivots)
            panel = jnp.dot(small, jnp.where(inside, unit, tops[l]), precision=hi, preferred_element_type=jnp.float32)
            out_ref[l, pl.ds(lo, block), :] = jnp.where(wide <= wide_row + lo, panel, 0.0)
            panels.append(panel)

        @pl.when(step < rank // block - 1)
        def _():
            for l in range(layers):
                work[l] = jnp.where(own, 0.0, work[l]) - lax.dot_general(
                    panels[l], panels[l], (((0,), (0,)), ((), ())), precision=hi, preferred_element_type=jnp.float32)

        return 0

    lax.fori_loop(0, rank // block, eliminate, 0)

def inverse_factor(gram):
    return pl.pallas_call(
        functools.partial(inverse_kernel, 32, 8),
        out_shape=jax.ShapeDtypeStruct(gram.shape, jnp.float32),
        in_specs=[pl.BlockSpec(memory_space=pltpu.VMEM)],
        out_specs=pl.BlockSpec(memory_space=pltpu.VMEM),
        scratch_shapes=[pltpu.VMEM(gram.shape, jnp.float32)],
        name="inverse_factor",
    )(gram)


def cross_kernel(part, here_ref, buffer_ref, power_ref, mine_ref, theirs_ref, whole):
    rest = power_ref[0]
    terms = []
    for _ in range(3):
        terms.append(rest.astype(jnp.bfloat16))
        rest = rest - terms[-1].astype(jnp.float32)
    total = lax.dot_general(
        buffer_ref[0],
        jnp.concatenate(terms, axis=1),
        (((0,), (0,)), ((), ())),
        preferred_element_type=jnp.float32,
    )
    rank = power_ref.shape[2]
    total = total[:, :rank] + (total[:, rank : 2 * rank] + total[:, 2 * rank :])
    padding = jnp.zeros((whole.shape[1] - part, whole.shape[2]), jnp.float32)
    for j in range(2 * Z_SIZE):
        whole[j] = jnp.concatenate([total[j * part : (j + 1) * part, :], padding], axis=0)
    z, core = here_ref[0], here_ref[1]
    for ref, owner in ((mine_ref, core), (theirs_ref, 1 - core)):
        for i in range(Z_SIZE):
            by = (1, 1, 2, 2, 3, 3, 4, 0)[i]
            place = lax.rem(z + by * (1 - 2 * owner) + Z_SIZE, Z_SIZE)
            whose = 1 - owner if i in (1, 3, 5) else owner
            ref[i, 0] = whole[2 * place + whose]


def cross(buffer16, power, padded):
    layers, rows, cols = buffer16.shape
    rank = power.shape[2]
    shape = jax.ShapeDtypeStruct((Z_SIZE, layers, padded, rank), jnp.float32)
    out_spec = pl.BlockSpec((Z_SIZE, 1, padded, rank), lambda l, here: (0, l, 0, 0))
    return pl.pallas_call(
        functools.partial(cross_kernel, cols // (2 * Z_SIZE)),
        out_shape=(shape, shape),
        grid_spec=pltpu.PrefetchScalarGridSpec(
            num_scalar_prefetch=1,
            grid=(layers,),
            in_specs=[
                pl.BlockSpec((1, rows, cols), lambda l, here: (l, 0, 0)),
                pl.BlockSpec((1, rows, rank), lambda l, here: (l, 0, 0)),
            ],
            out_specs=(out_spec, out_spec),
            scratch_shapes=[pltpu.VMEM((2 * Z_SIZE, padded, rank), jnp.float32)],
        ),
        name="cross",
    )(position(), buffer16, power)


def scatter_near(blocks):
    three, four, one = lax.optimization_barrier((blocks[4:6], blocks[6], blocks[0:2]))
    three, four, one = turn(three, 1), turn(four, 2), turn(one, 1)
    three, four, one = lax.optimization_barrier((three, four, one))
    two = jnp.stack([blocks[2] + three[0] + four, blocks[3] + three[1]])
    return blocks[7], one, two


def scatter_end(own, one, far):
    total = one + far
    total = jnp.stack([own + total[0], total[1]])
    other = swap(total, CORE, 2, 1)
    return jnp.stack([total[0] + other[1], total[1] + other[0]])


def shards(grad, momentum, basis):
    hi = lax.Precision.HIGHEST
    scale = math.sqrt(D * FF / RANK)
    layers, rows, cols = grad.shape
    tp = lax.axis_index(TP)
    part = basis.shape[0]
    padded = -(-part // 16) * 16

    def decay(_):
        buffer = MOMENTUM_DECAY * momentum.astype(jnp.float32) + grad.astype(jnp.float32)
        return buffer.astype(jnp.bfloat16)

    shard = jnp.pad(basis.transpose(1, 0, 2), ((0, 0), (0, padded - part), (0, 0)))
    pair = jnp.stack([shard, swap(shard, CORE, 2, 1)])
    pieces, buffer16 = gather_fsdp(pair, None, [decay])
    partial = lax.all_to_all(power_step(buffer16, pieces, part), TP, 0, 0, tiled=True)
    power = lax.all_gather(partial.sum(0), TP, axis=1).reshape(layers, rows, RANK)

    share = RANK // TP_SIZE
    gram = jnp.einsum("lmr,lms->lrs", power, power, precision=hi)
    gram = lax.dynamic_slice_in_dim(gram, tp * share, share, 1)
    gram, right = lax.optimization_barrier((gram, power))
    mine, theirs = cross(buffer16, right, padded)
    gram = gram + swap(gram, CORE, 2, 1)
    gram = add_crossing(add_two(add_one(gram)))
    mine = mine + swap(theirs, CORE, 2, 1)
    mine, gram = lax.optimization_barrier((mine, gram))
    hops = scatter_near(mine)

    gram = lax.all_gather(gram, TP, axis=1).reshape(layers, RANK, RANK)
    gram, *hops = lax.optimization_barrier((gram, *hops))
    own, one, two = hops
    far, inverse = lax.optimization_barrier((turn(two, 2), inverse_factor(gram)))
    mixed = scatter_end(own, one, far)
    ortho = jnp.einsum("lmr,lir->lmi", power, inverse, precision=hi).astype(jnp.bfloat16)

    project = jnp.einsum("clnr,lir->clni", mixed, inverse, precision=hi)
    colsq = jnp.sum(project * project, axis=2, keepdims=True)
    pieces, colsq = gather_fsdp(
        project.astype(jnp.bfloat16),
        colsq[0] + colsq[1],
        [
            functools.partial(add_square, X),
            functools.partial(add_square, Y),
            add_one,
            add_two,
            add_crossing,
        ],
    )
    norm = lax.rsqrt(colsq + EPSILON)
    basis_next = (project[0, :, :part] * norm).astype(jnp.bfloat16).transpose(1, 0, 2)
    momentum_next, update = finish(grad, momentum, ortho, norm, pieces, part, scale)
    return (momentum_next, basis_next, update)


def solution(mesh):
    torus = Mesh(mesh.devices.reshape(8, 2, 4, 4), FSDP + TP)
    return jax.shard_map(
        shards,
        mesh=torus,
        in_specs=(P(None, FSDP, TP), P(None, FSDP, TP), P(TP_FSDP, None, None)),
        out_specs=(P(None, FSDP, TP), P(TP_FSDP, None, None), P(None, FSDP, TP)),
        check_vma=False,
    )
```

```python
import functools
import math

import jax
import jax.numpy as jnp
from jax import lax
from jax.experimental import pallas as pl
from jax.experimental.pallas import tpu as pltpu
from jax.sharding import Mesh
from jax.sharding import PartitionSpec as P

D = 5120
FF = 27648
RANK = 256
LAYERS = 3
Z, CORE, X, Y = "fsdp_0", "fsdp_1", "tp_0", "tp_1"
FSDP = (Z, CORE)
TP = (X, Y)
TP_FSDP = TP + FSDP
Z_SIZE = 8
TP_SIZE = 16

MOMENTUM_DECAY = 0.8
EPSILON = 1e-06


def shift(value, axis, size, by):
    return lax.ppermute(value, axis, [(i, (i + by) % size) for i in range(size)])


def swap(value, axis, size, bit):
    return lax.ppermute(value, axis, [(i, i ^ bit) for i in range(size)])


def turn(value, by):
    pairs = []
    for z in range(Z_SIZE):
        pairs.append((2 * z, 2 * ((z + by) % Z_SIZE)))
        pairs.append((2 * z + 1, 2 * ((z - by) % Z_SIZE) + 1))
    return lax.ppermute(value, FSDP, pairs)


def position():
    return jnp.stack([lax.axis_index(Z), lax.axis_index(CORE)]).astype(jnp.int32)


def crossing(value):
    pairs = []
    for z in range(Z_SIZE):
        pairs.append((2 * z, 2 * ((z + 1) % Z_SIZE) + 1))
        pairs.append((2 * z + 1, 2 * ((z - 1) % Z_SIZE)))
    return lax.ppermute(value, FSDP, pairs)


def spin(value, axis, by, cores=0):
    pairs = []
    for i in range(4):
        pairs.append((i, (i + by) % 4 + 4 * cores))
        pairs.append((4 + i, (i - by) % 4 + 4 * (1 - cores)))
    return lax.ppermute(value, (CORE, axis), pairs)


def add_one(value):
    return value + turn(value, 1)


def add_two(value):
    return value + turn(value, 2)


def add_crossing(value):
    return value + crossing(value)


def add_four(axis, value):
    value = value + spin(value, axis, 1)
    return value + spin(value, axis, 1, 1)


RING_SEATS = (
    tuple((0, 0, i) for i in (0, 1)),
    tuple((0, 1 + i // 2, i % 2) for i in range(4)),
    tuple((0, -1 - i // 2, 1 - i % 2) for i in range(4)),
    tuple((0, 3 + i // 2, i % 2) for i in range(3)),
    tuple((0, -3 - i // 2, 1 - i % 2) for i in range(3)),
)
BOTH_SEATS = tuple(
    tuple((by, 0, other) for by in group)
    for group in ((0, 7, 1, 6, 2), (5, 3, 4))
    for other in (0, 1)
)


def gather_both(shard, busy):
    half = shard.shape[2] // 2
    left, right = shift(shard, Z, Z_SIZE, 1), shift(shard, Z, Z_SIZE, -1)
    left2, right2 = shift(shard, Z, Z_SIZE, 2), shift(shard, Z, Z_SIZE, -2)
    left2, right2, busy = lax.optimization_barrier((left2, right2, busy))
    left3, right3 = shift(left2, Z, Z_SIZE, 1), shift(right2, Z, Z_SIZE, -1)
    far_left = shift(left2[:, :, :half], Z, Z_SIZE, 2)
    far_right = shift(right2[:, :, half:], Z, Z_SIZE, -2)
    near = jnp.stack([shard, left, right, left2, right2])
    near2 = swap(near, CORE, 2, 1)
    far = jnp.stack([left3, right3, jnp.concatenate([far_left, far_right], axis=2)])
    far2 = swap(far, CORE, 2, 1)
    return (near, near2, far, far2), busy


def gather_fsdp(pair, side, stages):
    stages = list(stages)

    def hop(value, side):
        moved = turn(value, 1)
        if stages:
            moved, side = lax.optimization_barrier((moved, stages.pop(0)(side)))
        return moved, side

    one, side = hop(pair, side)
    two, side = hop(one, side)
    near = jnp.concatenate([one, two])
    near2 = swap(near, CORE, 2, 1)
    three, side = hop(two, side)
    four, side = hop(three[0], side)
    far = jnp.concatenate([three, four[None]])
    far2 = swap(far, CORE, 2, 1)
    for stage in stages:
        side = stage(side)
    return (pair, near, near2, far, far2), side


def join(rows, seats, here_ref, refs, layer, blocks):
    z, core = here_ref[0], here_ref[1]
    ahead = 2 * core - 1
    for ref, group in zip(refs, seats):
        for i, (by, way, other) in enumerate(group):
            place = lax.rem(z + by + way * ahead + Z_SIZE, Z_SIZE)
            whose = 1 - core if other else core
            blocks[2 * place + whose] = ref[i, layer].astype(jnp.float32)
    return jnp.concatenate([blocks[j][:rows, :] for j in range(2 * Z_SIZE)], axis=0)


def finish_kernel(rows, scale, here_ref, grad_ref, momentum_ref, ortho_ref, norm_ref, *refs):
    momentum_next_ref, update_ref, blocks = refs[-3:]
    whole = join(rows, RING_SEATS, here_ref, refs[:-3], 0, blocks).astype(jnp.bfloat16)
    ortho = ortho_ref[0]
    scaled = (ortho.astype(jnp.float32) * (scale * norm_ref[0])).astype(jnp.bfloat16)
    last = (((1,), (1,)), ((), ()))
    feedback = lax.dot_general(ortho, whole, last, preferred_element_type=jnp.float32)
    buffer = MOMENTUM_DECAY * momentum_ref[0].astype(jnp.float32) + grad_ref[0].astype(jnp.float32)
    momentum_next_ref[0] = (buffer - (1.0 - MOMENTUM_DECAY) * feedback).astype(jnp.bfloat16)
    update = lax.dot_general(scaled, whole, last, preferred_element_type=jnp.float32)
    update_ref[0] = update.astype(jnp.bfloat16)


def power_kernel(rows, here_ref, buffer_ref, *refs):
    out_ref, blocks = refs[-2:]
    whole = join(rows, BOTH_SEATS, here_ref, refs[:-2], 0, blocks).astype(jnp.bfloat16)
    product = jnp.dot(buffer_ref[0], whole, preferred_element_type=jnp.float32)
    share = out_ref.shape[2]
    for t in range(out_ref.shape[0]):
        out_ref[t, 0] = product[t * share : (t + 1) * share, :]


def piece_specs(pieces):
    return [
        pl.BlockSpec((p.shape[0], 1) + p.shape[2:], lambda l, here: (0, l, 0, 0)) for p in pieces
    ]


def finish(grad, momentum, ortho, norm, pieces, rows, scale):
    layers, height, cols = grad.shape
    padded, rank = pieces[0].shape[2:]
    shape = jax.ShapeDtypeStruct(grad.shape, grad.dtype)

    def spec(m, n):
        return pl.BlockSpec((1, m, n), lambda l, here: (l, 0, 0))

    return pl.pallas_call(
        functools.partial(finish_kernel, rows, scale),
        out_shape=(shape, shape),
        grid_spec=pltpu.PrefetchScalarGridSpec(
            num_scalar_prefetch=1,
            grid=(layers,),
            in_specs=[spec(height, cols), spec(height, cols), spec(height, rank), spec(1, rank)]
            + piece_specs(pieces),
            out_specs=(spec(height, cols), spec(height, cols)),
            scratch_shapes=[pltpu.VMEM((2 * Z_SIZE, padded, rank), jnp.float32)],
        ),
        name="finish",
    )(position(), grad, momentum, ortho, norm, *pieces)


def power_step(buffer16, pieces, rows):
    layers, height, cols = buffer16.shape
    padded, rank = pieces[0].shape[2:]
    share = height // TP_SIZE
    return pl.pallas_call(
        functools.partial(power_kernel, rows),
        out_shape=jax.ShapeDtypeStruct((TP_SIZE, layers, share, rank), jnp.float32),
        grid_spec=pltpu.PrefetchScalarGridSpec(
            num_scalar_prefetch=1,
            grid=(layers,),
            in_specs=[pl.BlockSpec((1, height, cols), lambda l, here: (l, 0, 0))]
            + piece_specs(pieces),
            out_specs=pl.BlockSpec((TP_SIZE, 1, share, rank), lambda l, here: (0, l, 0, 0)),
            scratch_shapes=[pltpu.VMEM((2 * Z_SIZE, padded, rank), jnp.float32)],
        ),
        name="power",
    )(position(), buffer16, *pieces)


def inverse_kernel(block, group, gram_ref, out_ref, work):
    layers, rank = gram_ref.shape[0], gram_ref.shape[1]
    hi = lax.Precision.HIGHEST
    row = lax.broadcasted_iota(jnp.int32, (block, block), 0)
    lane = lax.broadcasted_iota(jnp.int32, (block, block), 1)
    eye = (row == lane).astype(jnp.float32)
    row_id = lax.broadcasted_iota(jnp.int32, (block, 2 * block), 0)
    wide = lax.broadcasted_iota(jnp.int32, (block, rank), 1)
    wide_row = lax.broadcasted_iota(jnp.int32, (block, rank), 0)
    place = lax.broadcasted_iota(jnp.int32, (rank, rank), 1)
    work[...] = gram_ref[...]

    def eliminate(step, _):
        lo = pl.multiple_of(step * block, block)
        tops = [work[l, pl.ds(lo, block), :] for l in range(layers)]
        diag = [pltpu.roll(top, rank - lo, 1)[:, :block] for top in tops]
        tails = [jnp.concatenate([d, eye], axis=1) for d in diag]
        ready = [[] for _ in range(layers)]
        for first in range(0, block, group):
            cols = [
                [jnp.broadcast_to(tail[:, c : c + 1], tail.shape) for c in range(first, first + group)]
                for tail in tails
            ]
            below = row_id[first:, :]
            for j in range(group):
                for l in range(layers):
                    tail, col = tails[l], cols[l]
                    factor = jnp.where(below > first + j, col[j] * (1.0 / col[j][j : j + 1, :]), 0.0)
                    for later in range(j + 1, group):
                        col[later] = col[later] - factor * col[later][j : j + 1, :]
                    tails[l] = tail - factor * tail[j : j + 1, :]
            for l in range(layers):
                ready[l].append(tails[l][:group, :])
                tails[l] = tails[l][group:, :]
        mats = [jnp.concatenate(parts, axis=0) for parts in ready]
        inside = (wide >= lo) & (wide < lo + block)
        unit = (wide - lo == wide_row).astype(jnp.float32)
        panels = []
        own = (place >= lo) & (place < lo + block)
        for l in range(layers):
            mat = mats[l]
            pivots = jnp.sum(jnp.where(row == lane, mat[:, :block], 0.0), axis=1, keepdims=True)
            small = mat[:, block:] * lax.rsqrt(pivots)
            panel = jnp.dot(small, jnp.where(inside, unit, tops[l]), precision=hi, preferred_element_type=jnp.float32)
            out_ref[l, pl.ds(lo, block), :] = jnp.where(wide <= wide_row + lo, panel, 0.0)
            panels.append(panel)

        @pl.when(step < rank // block - 1)
        def _():
            for l in range(layers):
                work[l] = jnp.where(own, 0.0, work[l]) - lax.dot_general(
                    panels[l], panels[l], (((0,), (0,)), ((), ())), precision=hi, preferred_element_type=jnp.float32)

        return 0

    lax.fori_loop(0, rank // block, eliminate, 0)

def inverse_factor(gram):
    return pl.pallas_call(
        functools.partial(inverse_kernel, 32, 8),
        out_shape=jax.ShapeDtypeStruct(gram.shape, jnp.float32),
        in_specs=[pl.BlockSpec(memory_space=pltpu.VMEM)],
        out_specs=pl.BlockSpec(memory_space=pltpu.VMEM),
        scratch_shapes=[pltpu.VMEM(gram.shape, jnp.float32)],
        name="inverse_factor",
    )(gram)


def cross_kernel(part, here_ref, buffer_ref, power_ref, mine_ref, theirs_ref, whole):
    rest = power_ref[0]
    terms = []
    for _ in range(3):
        terms.append(rest.astype(jnp.bfloat16))
        rest = rest - terms[-1].astype(jnp.float32)
    total = lax.dot_general(
        buffer_ref[0],
        jnp.concatenate(terms, axis=1),
        (((0,), (0,)), ((), ())),
        preferred_element_type=jnp.float32,
    )
    rank = power_ref.shape[2]
    total = total[:, :rank] + (total[:, rank : 2 * rank] + total[:, 2 * rank :])
    padding = jnp.zeros((whole.shape[1] - part, whole.shape[2]), jnp.float32)
    for j in range(2 * Z_SIZE):
        whole[j] = jnp.concatenate([total[j * part : (j + 1) * part, :], padding], axis=0)
    z, core = here_ref[0], here_ref[1]
    for ref, owner in ((mine_ref, core), (theirs_ref, 1 - core)):
        for i in range(Z_SIZE):
            by = (1, 1, 3, 3, 2, 2, 4, 0)[i]
            place = lax.rem(z + by * (1 - 2 * owner) + Z_SIZE, Z_SIZE)
            whose = 1 - owner if i in (1, 3, 5) else owner
            ref[i, 0] = whole[2 * place + whose]


def cross(buffer16, power, padded):
    layers, rows, cols = buffer16.shape
    rank = power.shape[2]
    shape = jax.ShapeDtypeStruct((Z_SIZE, layers, padded, rank), jnp.float32)
    out_spec = pl.BlockSpec((Z_SIZE, 1, padded, rank), lambda l, here: (0, l, 0, 0))
    return pl.pallas_call(
        functools.partial(cross_kernel, cols // (2 * Z_SIZE)),
        out_shape=(shape, shape),
        grid_spec=pltpu.PrefetchScalarGridSpec(
            num_scalar_prefetch=1,
            grid=(layers,),
            in_specs=[
                pl.BlockSpec((1, rows, cols), lambda l, here: (l, 0, 0)),
                pl.BlockSpec((1, rows, rank), lambda l, here: (l, 0, 0)),
            ],
            out_specs=(out_spec, out_spec),
            scratch_shapes=[pltpu.VMEM((2 * Z_SIZE, padded, rank), jnp.float32)],
        ),
        cost_estimate=pl.CostEstimate(
            flops=6 * layers * rows * cols * rank,
            bytes_accessed=2 * layers * rows * cols + 16 * layers * Z_SIZE * padded * rank,
            transcendentals=0,
        ),
        name="cross",
    )(position(), buffer16, power)


def scatter_near(blocks):
    next_, four = lax.optimization_barrier((blocks[0:4], blocks[6]))
    next_, four = lax.optimization_barrier((turn(next_, 1), turn(four, 2)))
    two = jnp.stack([blocks[4] + next_[2] + four, blocks[5] + next_[3]])
    return blocks[7], next_[0:2], two


def scatter_end(own, one, far):
    total = one + far
    total = jnp.stack([own + total[0], total[1]])
    other = swap(total, CORE, 2, 1)
    return jnp.stack([total[0] + other[1], total[1] + other[0]])


def shards(grad, momentum, basis):
    hi = lax.Precision.HIGHEST
    scale = math.sqrt(D * FF / RANK)
    layers, rows, cols = grad.shape
    tp = lax.axis_index(TP)
    part = basis.shape[0]
    padded = -(-part // 16) * 16

    buffer = MOMENTUM_DECAY * momentum.astype(jnp.float32) + grad.astype(jnp.float32)
    shard = jnp.pad(basis.transpose(1, 0, 2), ((0, 0), (0, padded - part), (0, 0)))
    pieces, buffer16 = gather_both(shard, buffer.astype(jnp.bfloat16))
    partial = lax.all_to_all(power_step(buffer16, pieces, part), TP, 0, 0, tiled=True)
    power = lax.all_gather(partial.sum(0), TP, axis=1).reshape(layers, rows, RANK)

    share = RANK // TP_SIZE
    gram = jnp.einsum("lmr,lms->lrs", power, power, precision=hi)
    gram = lax.dynamic_slice_in_dim(gram, tp * share, share, 1)
    gram = gram + swap(gram, CORE, 2, 1)
    gram, right = lax.optimization_barrier((gram, power))
    mine, theirs = cross(buffer16, right, padded)
    theirs, gram = lax.optimization_barrier((theirs, add_one(gram)))
    gram = add_crossing(add_two(gram))
    mine = mine + swap(theirs, CORE, 2, 1)
    mine, gram = lax.optimization_barrier((mine, gram))
    hops = scatter_near(mine)

    gram = lax.all_gather(gram, TP, axis=1).reshape(layers, RANK, RANK)
    gram, hops = lax.optimization_barrier((gram, hops))
    own, one, two = hops
    far, inverse = lax.optimization_barrier((turn(two, 2), inverse_factor(gram)))
    mixed = scatter_end(own, one, far)
    ortho = jnp.einsum("lmr,lir->lmi", power, inverse, precision=hi).astype(jnp.bfloat16)

    project = jnp.einsum("clnr,lir->clni", mixed, inverse, precision=hi)
    colsq = jnp.sum(project * project, axis=2, keepdims=True)
    pieces, colsq = gather_fsdp(
        project.astype(jnp.bfloat16),
        colsq[0] + colsq[1],
        [
            functools.partial(add_four, X),
            functools.partial(add_four, Y),
            add_one,
            add_two,
            add_crossing,
        ],
    )
    norm = lax.rsqrt(colsq + EPSILON)
    basis_next = (project[0, :, :part] * norm).astype(jnp.bfloat16).transpose(1, 0, 2)
    momentum_next, update = finish(grad, momentum, ortho, norm, pieces, part, scale)
    return (momentum_next, basis_next, update)


def solution(mesh):
    torus = Mesh(mesh.devices.reshape(8, 2, 4, 4), FSDP + TP)
    return jax.shard_map(
        shards,
        mesh=torus,
        in_specs=(P(None, FSDP, TP), P(None, FSDP, TP), P(TP_FSDP, None, None)),
        out_specs=(P(None, FSDP, TP), P(TP_FSDP, None, None), P(None, FSDP, TP)),
        check_vma=False,
    )
```

```python
import functools
import math

import jax
import jax.numpy as jnp
from jax import lax
from jax.experimental import pallas as pl
from jax.experimental.pallas import tpu as pltpu
from jax.sharding import Mesh
from jax.sharding import PartitionSpec as P

D = 5120
FF = 27648
RANK = 256
LAYERS = 3
Z, CORE, X, Y = "fsdp_0", "fsdp_1", "tp_0", "tp_1"
FSDP = (Z, CORE)
TP = (X, Y)
TP_FSDP = TP + FSDP
Z_SIZE = 8
TP_SIZE = 16

MOMENTUM_DECAY = 0.8
EPSILON = 1e-06


def shift(value, axis, size, by):
    return lax.ppermute(value, axis, [(i, (i + by) % size) for i in range(size)])


def swap(value, axis, size, bit):
    return lax.ppermute(value, axis, [(i, i ^ bit) for i in range(size)])


def turn(value, by):
    pairs = []
    for z in range(Z_SIZE):
        pairs.append((2 * z, 2 * ((z + by) % Z_SIZE)))
        pairs.append((2 * z + 1, 2 * ((z - by) % Z_SIZE) + 1))
    return lax.ppermute(value, FSDP, pairs)


def position():
    return jnp.stack([lax.axis_index(axis) for axis in (Z, CORE, X)]).astype(jnp.int32)


def crossing(value):
    pairs = []
    for z in range(Z_SIZE):
        pairs.append((2 * z, 2 * ((z + 1) % Z_SIZE) + 1))
        pairs.append((2 * z + 1, 2 * ((z - 1) % Z_SIZE)))
    return lax.ppermute(value, FSDP, pairs)


def spin(value, axis, by, cores=0):
    pairs = []
    for i in range(4):
        pairs.append((i, (i + by) % 4 + 4 * cores))
        pairs.append((4 + i, (i - by) % 4 + 4 * (1 - cores)))
    return lax.ppermute(value, (CORE, axis), pairs)


X_SEATS = (0, 3, 1, 2)


def gather_four(value, axis):
    return [value, shift(value, axis, 4, 1), shift(value, axis, 4, -1), shift(value, axis, 4, 2)]


def in_order(value, here_ref, blocks):
    height = value.shape[0] // 4
    for i, by in enumerate(X_SEATS):
        blocks[lax.rem(here_ref[2] + by, 4)] = value[i * height : (i + 1) * height, :]
    return blocks[...].reshape(value.shape)


def add_one(value):
    return value + turn(value, 1)


def add_two(value):
    return value + turn(value, 2)


def add_crossing(value):
    return value + crossing(value)


def add_four(axis, value):
    value = value + spin(value, axis, 1)
    return value + spin(value, axis, 1, 1)


RING_SEATS = (
    tuple((0, 0, i) for i in (0, 1)),
    tuple((0, 1 + i // 2, i % 2) for i in range(4)),
    tuple((0, -1 - i // 2, 1 - i % 2) for i in range(4)),
    tuple((0, 3 + i // 2, i % 2) for i in range(3)),
    tuple((0, -3 - i // 2, 1 - i % 2) for i in range(3)),
)
BOTH_SEATS = tuple(
    tuple((by, 0, other) for by in group)
    for group in ((0, 7, 1, 6, 2), (5, 3, 4))
    for other in (0, 1)
)


def gather_both(shard):
    half = shard.shape[2] // 2
    left, right = shift(shard, Z, Z_SIZE, 1), shift(shard, Z, Z_SIZE, -1)
    left2, right2 = shift(shard, Z, Z_SIZE, 2), shift(shard, Z, Z_SIZE, -2)
    left3, right3 = shift(left2, Z, Z_SIZE, 1), shift(right2, Z, Z_SIZE, -1)
    far_left = shift(left2[:, :, :half], Z, Z_SIZE, 2)
    far_right = shift(right2[:, :, half:], Z, Z_SIZE, -2)
    near = jnp.stack([shard, left, right, left2, right2])
    near2 = swap(near, CORE, 2, 1)
    far = jnp.stack([left3, right3, jnp.concatenate([far_left, far_right], axis=2)])
    far2 = swap(far, CORE, 2, 1)
    return near, near2, far, far2


def gather_fsdp(pair, side, stages):
    stages = list(stages)

    def hop(value, side):
        moved = turn(value, 1)
        if stages:
            moved, side = lax.optimization_barrier((moved, stages.pop(0)(side)))
        return moved, side

    one, side = hop(pair, side)
    two, side = hop(one, side)
    near = jnp.concatenate([one, two])
    near2 = swap(near, CORE, 2, 1)
    three, side = hop(two, side)
    four, side = hop(three[0], side)
    far = jnp.concatenate([three, four[None]])
    far2 = swap(far, CORE, 2, 1)
    for stage in stages:
        side = stage(side)
    return (pair, near, near2, far, far2), side


def join(rows, seats, here_ref, refs, layer, blocks):
    z, core = here_ref[0], here_ref[1]
    ahead = 2 * core - 1
    for ref, group in zip(refs, seats):
        for i, (by, way, other) in enumerate(group):
            place = lax.rem(z + by + way * ahead + Z_SIZE, Z_SIZE)
            whose = 1 - core if other else core
            blocks[2 * place + whose] = ref[i, layer].astype(jnp.float32)
    return jnp.concatenate([blocks[j][:rows, :] for j in range(2 * Z_SIZE)], axis=0)


def finish_kernel(rows, scale, here_ref, grad_ref, momentum_ref, ortho_ref, norm_ref, *refs):
    momentum_next_ref, update_ref, blocks, ordered = refs[-4:]
    whole = join(rows, RING_SEATS, here_ref, refs[:-4], 0, blocks).astype(jnp.bfloat16)
    ortho = in_order(ortho_ref[0], here_ref, ordered)
    scaled = (ortho.astype(jnp.float32) * (scale * norm_ref[0])).astype(jnp.bfloat16)
    last = (((1,), (1,)), ((), ()))
    feedback = lax.dot_general(ortho, whole, last, preferred_element_type=jnp.float32)
    buffer = MOMENTUM_DECAY * momentum_ref[0].astype(jnp.float32) + grad_ref[0].astype(jnp.float32)
    momentum_next_ref[0] = (buffer - (1.0 - MOMENTUM_DECAY) * feedback).astype(jnp.bfloat16)
    update = lax.dot_general(scaled, whole, last, preferred_element_type=jnp.float32)
    update_ref[0] = update.astype(jnp.bfloat16)


def power_kernel(rows, here_ref, buffer_ref, *refs):
    out_ref, blocks = refs[-2:]
    whole = join(rows, BOTH_SEATS, here_ref, refs[:-2], 0, blocks).astype(jnp.bfloat16)
    product = jnp.dot(buffer_ref[0], whole, preferred_element_type=jnp.float32)
    share = out_ref.shape[2]
    for t in range(out_ref.shape[0]):
        out_ref[t, 0] = product[t * share : (t + 1) * share, :]


def piece_specs(pieces):
    return [
        pl.BlockSpec((p.shape[0], 1) + p.shape[2:], lambda l, here: (0, l, 0, 0)) for p in pieces
    ]


def finish(grad, momentum, ortho, norm, pieces, rows, scale):
    layers, height, cols = grad.shape
    padded, rank = pieces[0].shape[2:]
    shape = jax.ShapeDtypeStruct(grad.shape, grad.dtype)

    def spec(m, n):
        return pl.BlockSpec((1, m, n), lambda l, here: (l, 0, 0))

    return pl.pallas_call(
        functools.partial(finish_kernel, rows, scale),
        out_shape=(shape, shape),
        grid_spec=pltpu.PrefetchScalarGridSpec(
            num_scalar_prefetch=1,
            grid=(layers,),
            in_specs=[spec(height, cols), spec(height, cols), spec(height, rank), spec(1, rank)]
            + piece_specs(pieces),
            out_specs=(spec(height, cols), spec(height, cols)),
            scratch_shapes=[
                pltpu.VMEM((2 * Z_SIZE, padded, rank), jnp.float32),
                pltpu.VMEM((4, height // 4, rank), ortho.dtype),
            ],
        ),
        name="finish",
    )(position(), grad, momentum, ortho, norm, *pieces)


def power_step(buffer16, pieces, rows):
    layers, height, cols = buffer16.shape
    padded, rank = pieces[0].shape[2:]
    share = height // 4
    return pl.pallas_call(
        functools.partial(power_kernel, rows),
        out_shape=jax.ShapeDtypeStruct((4, layers, share, rank), jnp.float32),
        grid_spec=pltpu.PrefetchScalarGridSpec(
            num_scalar_prefetch=1,
            grid=(layers,),
            in_specs=[pl.BlockSpec((1, height, cols), lambda l, here: (l, 0, 0))]
            + piece_specs(pieces),
            out_specs=pl.BlockSpec((4, 1, share, rank), lambda l, here: (0, l, 0, 0)),
            scratch_shapes=[pltpu.VMEM((2 * Z_SIZE, padded, rank), jnp.float32)],
        ),
        name="power",
    )(position(), buffer16, *pieces)


def inverse_kernel(block, group, gram_ref, out_ref, work):
    layers, rank = gram_ref.shape[0], gram_ref.shape[1]
    hi = lax.Precision.HIGHEST
    row = lax.broadcasted_iota(jnp.int32, (block, block), 0)
    lane = lax.broadcasted_iota(jnp.int32, (block, block), 1)
    eye = (row == lane).astype(jnp.float32)
    row_id = lax.broadcasted_iota(jnp.int32, (block, 2 * block), 0)
    wide = lax.broadcasted_iota(jnp.int32, (block, rank), 1)
    wide_row = lax.broadcasted_iota(jnp.int32, (block, rank), 0)
    place = lax.broadcasted_iota(jnp.int32, (rank, rank), 1)
    work[...] = gram_ref[...]

    def eliminate(step, _):
        lo = pl.multiple_of(step * block, block)
        tops = [work[l, pl.ds(lo, block), :] for l in range(layers)]
        diag = [pltpu.roll(top, rank - lo, 1)[:, :block] for top in tops]
        tails = [jnp.concatenate([d, eye], axis=1) for d in diag]
        ready = [[] for _ in range(layers)]
        for first in range(0, block, group):
            cols = [
                [jnp.broadcast_to(tail[:, c : c + 1], tail.shape) for c in range(first, first + group)]
                for tail in tails
            ]
            below = row_id[first:, :]
            for j in range(group):
                for l in range(layers):
                    tail, col = tails[l], cols[l]
                    factor = jnp.where(below > first + j, col[j] * (1.0 / col[j][j : j + 1, :]), 0.0)
                    for later in range(j + 1, group):
                        col[later] = col[later] - factor * col[later][j : j + 1, :]
                    tails[l] = tail - factor * tail[j : j + 1, :]
            for l in range(layers):
                ready[l].append(tails[l][:group, :])
                tails[l] = tails[l][group:, :]
        mats = [jnp.concatenate(parts, axis=0) for parts in ready]
        inside = (wide >= lo) & (wide < lo + block)
        unit = (wide - lo == wide_row).astype(jnp.float32)
        panels = []
        own = (place >= lo) & (place < lo + block)
        for l in range(layers):
            mat = mats[l]
            pivots = jnp.sum(jnp.where(row == lane, mat[:, :block], 0.0), axis=1, keepdims=True)
            small = mat[:, block:] * lax.rsqrt(pivots)
            panel = jnp.dot(small, jnp.where(inside, unit, tops[l]), precision=hi, preferred_element_type=jnp.float32)
            out_ref[l, pl.ds(lo, block), :] = jnp.where(wide <= wide_row + lo, panel, 0.0)
            panels.append(panel)

        @pl.when(step < rank // block - 1)
        def _():
            for l in range(layers):
                work[l] = jnp.where(own, 0.0, work[l]) - lax.dot_general(
                    panels[l], panels[l], (((0,), (0,)), ((), ())), precision=hi, preferred_element_type=jnp.float32)

        return 0

    lax.fori_loop(0, rank // block, eliminate, 0)

def inverse_factor(gram):
    return pl.pallas_call(
        functools.partial(inverse_kernel, 32, 8),
        out_shape=jax.ShapeDtypeStruct(gram.shape, jnp.float32),
        in_specs=[pl.BlockSpec(memory_space=pltpu.VMEM)],
        out_specs=pl.BlockSpec(memory_space=pltpu.VMEM),
        scratch_shapes=[pltpu.VMEM(gram.shape, jnp.float32)],
        name="inverse_factor",
    )(gram)


def cross_kernel(part, here_ref, buffer_ref, power_ref, mine_ref, theirs_ref, whole, ordered):
    rest = in_order(power_ref[0], here_ref, ordered)
    terms = []
    for _ in range(3):
        terms.append(rest.astype(jnp.bfloat16))
        rest = rest - terms[-1].astype(jnp.float32)
    total = lax.dot_general(
        buffer_ref[0],
        jnp.concatenate(terms, axis=1),
        (((0,), (0,)), ((), ())),
        preferred_element_type=jnp.float32,
    )
    rank = power_ref.shape[2]
    total = total[:, :rank] + (total[:, rank : 2 * rank] + total[:, 2 * rank :])
    padding = jnp.zeros((whole.shape[1] - part, whole.shape[2]), jnp.float32)
    for j in range(2 * Z_SIZE):
        whole[j] = jnp.concatenate([total[j * part : (j + 1) * part, :], padding], axis=0)
    z, core = here_ref[0], here_ref[1]
    for ref, owner in ((mine_ref, core), (theirs_ref, 1 - core)):
        for i in range(Z_SIZE):
            by = (1, 1, 3, 3, 2, 2, 4, 0)[i]
            place = lax.rem(z + by * (1 - 2 * owner) + Z_SIZE, Z_SIZE)
            whose = 1 - owner if i in (1, 3, 5) else owner
            ref[i, 0] = whole[2 * place + whose]


def cross(buffer16, power, padded):
    layers, rows, cols = buffer16.shape
    rank = power.shape[2]
    shape = jax.ShapeDtypeStruct((Z_SIZE, layers, padded, rank), jnp.float32)
    out_spec = pl.BlockSpec((Z_SIZE, 1, padded, rank), lambda l, here: (0, l, 0, 0))
    return pl.pallas_call(
        functools.partial(cross_kernel, cols // (2 * Z_SIZE)),
        out_shape=(shape, shape),
        grid_spec=pltpu.PrefetchScalarGridSpec(
            num_scalar_prefetch=1,
            grid=(layers,),
            in_specs=[
                pl.BlockSpec((1, rows, cols), lambda l, here: (l, 0, 0)),
                pl.BlockSpec((1, rows, rank), lambda l, here: (l, 0, 0)),
            ],
            out_specs=(out_spec, out_spec),
            scratch_shapes=[
                pltpu.VMEM((2 * Z_SIZE, padded, rank), jnp.float32),
                pltpu.VMEM((4, rows // 4, rank), jnp.float32),
            ],
        ),
        cost_estimate=pl.CostEstimate(
            flops=6 * layers * rows * cols * rank,
            bytes_accessed=2 * layers * rows * cols + 16 * layers * Z_SIZE * padded * rank,
            transcendentals=0,
        ),
        name="cross",
    )(position(), buffer16, power)


def scatter_near(mine, theirs):
    next_, four = lax.optimization_barrier((mine[0:4] + theirs[0:4], mine[6] + theirs[6]))
    next_, four = lax.optimization_barrier((turn(next_, 1), turn(four, 2)))
    two = mine[4:6] + theirs[4:6]
    two = jnp.stack([two[0] + next_[2] + four, two[1] + next_[3]])
    return mine[7] + theirs[7], next_[0:2], two


def scatter_end(own, one, far):
    total = one + far
    total = jnp.stack([own + total[0], total[1]])
    other = swap(total, CORE, 2, 1)
    return jnp.stack([total[0] + other[1], total[1] + other[0]])


def shards(grad, momentum, basis):
    hi = lax.Precision.HIGHEST
    scale = math.sqrt(D * FF / RANK)
    layers, rows, cols = grad.shape
    tp = lax.axis_index(TP)
    part = basis.shape[0]
    padded = -(-part // 16) * 16

    buffer = MOMENTUM_DECAY * momentum.astype(jnp.float32) + grad.astype(jnp.float32)
    shard = jnp.pad(basis.transpose(1, 0, 2), ((0, 0), (0, padded - part), (0, 0)))
    buffer16 = buffer.astype(jnp.bfloat16)
    pieces = gather_both(shard)
    partial = lax.all_to_all(power_step(buffer16, pieces, part), X, 0, 0, tiled=True).sum(0)
    power = jnp.concatenate(gather_four(sum(gather_four(partial, Y)), X), axis=1)

    share = RANK // TP_SIZE
    gram = jnp.einsum("lmr,lms->lrs", power, power, precision=hi)
    gram = lax.dynamic_slice_in_dim(gram, tp * share, share, 1)
    gram = gram + swap(gram, CORE, 2, 1)
    gram, right = lax.optimization_barrier((gram, power))
    mine, theirs = cross(buffer16, right, padded)
    theirs, gram = lax.optimization_barrier((theirs, add_one(gram)))
    gram = add_crossing(add_two(gram))
    mine, theirs, gram = lax.optimization_barrier((mine, swap(theirs, CORE, 2, 1), gram))
    hops = scatter_near(mine, theirs)

    gram = lax.all_gather(gram, TP, axis=1).reshape(layers, RANK, RANK)
    gram, hops = lax.optimization_barrier((gram, hops))
    own, one, two = hops
    far, inverse = lax.optimization_barrier((turn(two, 2), inverse_factor(gram)))
    mixed = scatter_end(own, one, far)
    ortho = jnp.einsum("lmr,lir->lmi", power, inverse, precision=hi).astype(jnp.bfloat16)

    project = jnp.einsum("clnr,lir->clni", mixed, inverse, precision=hi)
    colsq = jnp.sum(project * project, axis=2, keepdims=True)
    pieces, colsq = gather_fsdp(
        project.astype(jnp.bfloat16),
        colsq[0] + colsq[1],
        [
            functools.partial(add_four, X),
            functools.partial(add_four, Y),
            add_one,
            add_two,
            add_crossing,
        ],
    )
    norm = lax.rsqrt(colsq + EPSILON)
    basis_next = (project[0, :, :part] * norm).astype(jnp.bfloat16).transpose(1, 0, 2)
    momentum_next, update = finish(grad, momentum, ortho, norm, pieces, part, scale)
    return (momentum_next, basis_next, update)


def solution(mesh):
    torus = Mesh(mesh.devices.reshape(8, 2, 4, 4), FSDP + TP)
    return jax.shard_map(
        shards,
        mesh=torus,
        in_specs=(P(None, FSDP, TP), P(None, FSDP, TP), P(TP_FSDP, None, None)),
        out_specs=(P(None, FSDP, TP), P(TP_FSDP, None, None), P(None, FSDP, TP)),
        check_vma=False,
    )
```

```python
import functools
import math

import jax
import jax.numpy as jnp
from jax import lax
from jax.experimental import pallas as pl
from jax.experimental.pallas import tpu as pltpu
from jax.sharding import Mesh
from jax.sharding import PartitionSpec as P

D = 5120
FF = 27648
RANK = 256
LAYERS = 3
Z, CORE, X, Y = "fsdp_0", "fsdp_1", "tp_0", "tp_1"
FSDP = (Z, CORE)
TP = (X, Y)
TP_FSDP = TP + FSDP
Z_SIZE = 8
TP_SIZE = 16

MOMENTUM_DECAY = 0.8
EPSILON = 1e-06


def shift(value, axis, size, by):
    return lax.ppermute(value, axis, [(i, (i + by) % size) for i in range(size)])


def swap(value, axis, size, bit):
    return lax.ppermute(value, axis, [(i, i ^ bit) for i in range(size)])


def turn(value, by):
    pairs = []
    for z in range(Z_SIZE):
        pairs.append((2 * z, 2 * ((z + by) % Z_SIZE)))
        pairs.append((2 * z + 1, 2 * ((z - by) % Z_SIZE) + 1))
    return lax.ppermute(value, FSDP, pairs)


def position():
    return jnp.stack([lax.axis_index(Z), lax.axis_index(CORE)]).astype(jnp.int32)


def crossing(value):
    pairs = []
    for z in range(Z_SIZE):
        pairs.append((2 * z, 2 * ((z + 1) % Z_SIZE) + 1))
        pairs.append((2 * z + 1, 2 * ((z - 1) % Z_SIZE)))
    return lax.ppermute(value, FSDP, pairs)


def spin(value, axis, by, cores=0):
    pairs = []
    for i in range(4):
        pairs.append((i, (i + by) % 4 + 4 * cores))
        pairs.append((4 + i, (i - by) % 4 + 4 * (1 - cores)))
    return lax.ppermute(value, (CORE, axis), pairs)


def add_one(value):
    return value + turn(value, 1)


def add_two(value):
    return value + turn(value, 2)


def add_crossing(value):
    return value + crossing(value)


def add_four(axis, value):
    value = value + spin(value, axis, 1)
    return value + spin(value, axis, 1, 1)


RING_SEATS = (
    tuple((0, 0, i) for i in (0, 1)),
    tuple((0, 1 + i // 2, i % 2) for i in range(4)),
    tuple((0, -1 - i // 2, 1 - i % 2) for i in range(4)),
    tuple((0, 3 + i // 2, i % 2) for i in range(3)),
    tuple((0, -3 - i // 2, 1 - i % 2) for i in range(3)),
)
BOTH_SEATS = tuple(
    tuple((by, 0, other) for by in group)
    for group in ((0, 7, 1, 6, 2), (5, 3, 4))
    for other in (0, 1)
)


def gather_both(shard, busy):
    half = shard.shape[2] // 2
    left, right = shift(shard, Z, Z_SIZE, 1), shift(shard, Z, Z_SIZE, -1)
    left2, right2 = shift(shard, Z, Z_SIZE, 2), shift(shard, Z, Z_SIZE, -2)
    left3, right3 = shift(left2, Z, Z_SIZE, 1), shift(right2, Z, Z_SIZE, -1)
    far_left = shift(left2[:, :, :half], Z, Z_SIZE, 2)
    far_right = shift(right2[:, :, half:], Z, Z_SIZE, -2)
    left3, right3, far_left, far_right, busy = lax.optimization_barrier(
        (left3, right3, far_left, far_right, busy)
    )
    near = jnp.stack([shard, left, right, left2, right2])
    near2 = swap(near, CORE, 2, 1)
    far = jnp.stack([left3, right3, jnp.concatenate([far_left, far_right], axis=2)])
    far2 = swap(far, CORE, 2, 1)
    return (near, near2, far, far2), busy


def gather_fsdp(pair, side, first, second, last):
    one, two, side = lax.optimization_barrier((turn(pair, 1), turn(pair, 2), first(side)))
    three, four = turn(two, 1), turn(two[0], 2)
    near = jnp.concatenate([one, two])
    near2 = swap(near, CORE, 2, 1)
    three, four, side = lax.optimization_barrier((three, four, second(side)))
    far = jnp.concatenate([three, four[None]])
    far2 = swap(far, CORE, 2, 1)
    return (pair, near, near2, far, far2), last(side)


def join(rows, seats, here_ref, refs, layer, blocks):
    z, core = here_ref[0], here_ref[1]
    ahead = 2 * core - 1
    for ref, group in zip(refs, seats):
        for i, (by, way, other) in enumerate(group):
            place = lax.rem(z + by + way * ahead + Z_SIZE, Z_SIZE)
            whose = 1 - core if other else core
            blocks[2 * place + whose] = ref[i, layer].astype(jnp.float32)
    return jnp.concatenate([blocks[j][:rows, :] for j in range(2 * Z_SIZE)], axis=0)


def finish_kernel(rows, scale, here_ref, grad_ref, momentum_ref, ortho_ref, norm_ref, *refs):
    momentum_next_ref, update_ref, blocks = refs[-3:]
    whole = join(rows, RING_SEATS, here_ref, refs[:-3], 0, blocks).astype(jnp.bfloat16)
    ortho = ortho_ref[0]
    scaled = (ortho.astype(jnp.float32) * (scale * norm_ref[0])).astype(jnp.bfloat16)
    both = lax.dot_general(
        jnp.concatenate([ortho, scaled], axis=0),
        whole,
        (((1,), (1,)), ((), ())),
        preferred_element_type=jnp.float32,
    )
    height = ortho.shape[0]
    feedback, update = both[:height, :], both[height:, :]
    buffer = MOMENTUM_DECAY * momentum_ref[0].astype(jnp.float32) + grad_ref[0].astype(jnp.float32)
    momentum_next_ref[0] = (buffer - (1.0 - MOMENTUM_DECAY) * feedback).astype(jnp.bfloat16)
    update_ref[0] = update.astype(jnp.bfloat16)


def power_kernel(rows, here_ref, buffer_ref, *refs):
    out_ref, blocks = refs[-2:]
    whole = join(rows, BOTH_SEATS, here_ref, refs[:-2], 0, blocks).astype(jnp.bfloat16)
    product = jnp.dot(buffer_ref[0], whole, preferred_element_type=jnp.float32)
    share = out_ref.shape[2]
    for t in range(out_ref.shape[0]):
        out_ref[t, 0] = product[t * share : (t + 1) * share, :]


def piece_specs(pieces):
    return [
        pl.BlockSpec((p.shape[0], 1) + p.shape[2:], lambda *ids: (0, ids[0], 0, 0)) for p in pieces
    ]


def finish(grad, momentum, ortho, norm, pieces, rows, scale):
    layers, height, cols = grad.shape
    padded, rank = pieces[0].shape[2:]
    shape = jax.ShapeDtypeStruct(grad.shape, grad.dtype)

    def spec(m, n):
        return pl.BlockSpec((1, m, n), lambda l, here: (l, 0, 0))

    return pl.pallas_call(
        functools.partial(finish_kernel, rows, scale),
        out_shape=(shape, shape),
        grid_spec=pltpu.PrefetchScalarGridSpec(
            num_scalar_prefetch=1,
            grid=(layers,),
            in_specs=[spec(height, cols), spec(height, cols), spec(height, rank), spec(1, rank)]
            + piece_specs(pieces),
            out_specs=(spec(height, cols), spec(height, cols)),
            scratch_shapes=[pltpu.VMEM((2 * Z_SIZE, padded, rank), jnp.float32)],
        ),
        name="finish",
    )(position(), grad, momentum, ortho, norm, *pieces)


def power_step(buffer16, pieces, rows):
    layers, height, cols = buffer16.shape
    padded, rank = pieces[0].shape[2:]
    share = height // TP_SIZE
    return pl.pallas_call(
        functools.partial(power_kernel, rows),
        out_shape=jax.ShapeDtypeStruct((TP_SIZE, layers, share, rank), jnp.float32),
        grid_spec=pltpu.PrefetchScalarGridSpec(
            num_scalar_prefetch=1,
            grid=(layers,),
            in_specs=[pl.BlockSpec((1, height, cols), lambda l, here: (l, 0, 0))]
            + piece_specs(pieces),
            out_specs=pl.BlockSpec((TP_SIZE, 1, share, rank), lambda l, here: (0, l, 0, 0)),
            scratch_shapes=[pltpu.VMEM((2 * Z_SIZE, padded, rank), jnp.float32)],
        ),
        name="power",
    )(position(), buffer16, *pieces)


def inverse_kernel(block, group, gram_ref, out_ref, work):
    layers, rank = gram_ref.shape[0], gram_ref.shape[1]
    hi = lax.Precision.HIGHEST
    row = lax.broadcasted_iota(jnp.int32, (block, block), 0)
    lane = lax.broadcasted_iota(jnp.int32, (block, block), 1)
    eye = (row == lane).astype(jnp.float32)
    row_id = lax.broadcasted_iota(jnp.int32, (block, 2 * block), 0)
    wide = lax.broadcasted_iota(jnp.int32, (block, rank), 1)
    wide_row = lax.broadcasted_iota(jnp.int32, (block, rank), 0)
    place = lax.broadcasted_iota(jnp.int32, (rank, rank), 1)
    work[...] = gram_ref[...]

    def eliminate(step, _):
        lo = pl.multiple_of(step * block, block)
        tops = [work[l, pl.ds(lo, block), :] for l in range(layers)]
        diag = [pltpu.roll(top, rank - lo, 1)[:, :block] for top in tops]
        tails = [jnp.concatenate([d, eye], axis=1) for d in diag]
        ready = [[] for _ in range(layers)]
        for first in range(0, block, group):
            cols = [
                [jnp.broadcast_to(tail[:, c : c + 1], tail.shape) for c in range(first, first + group)]
                for tail in tails
            ]
            below = row_id[first:, :]
            for j in range(group):
                for l in range(layers):
                    tail, col = tails[l], cols[l]
                    factor = jnp.where(below > first + j, col[j] * (1.0 / col[j][j : j + 1, :]), 0.0)
                    for later in range(j + 1, group):
                        col[later] = col[later] - factor * col[later][j : j + 1, :]
                    tails[l] = tail - factor * tail[j : j + 1, :]
            for l in range(layers):
                ready[l].append(tails[l][:group, :])
                tails[l] = tails[l][group:, :]
        mats = [jnp.concatenate(parts, axis=0) for parts in ready]
        inside = (wide >= lo) & (wide < lo + block)
        unit = (wide - lo == wide_row).astype(jnp.float32)
        panels = []
        own = (place >= lo) & (place < lo + block)
        for l in range(layers):
            mat = mats[l]
            pivots = jnp.sum(jnp.where(row == lane, mat[:, :block], 0.0), axis=1, keepdims=True)
            small = mat[:, block:] * lax.rsqrt(pivots)
            panel = jnp.dot(small, jnp.where(inside, unit, tops[l]), precision=hi, preferred_element_type=jnp.float32)
            out_ref[l, pl.ds(lo, block), :] = jnp.where(wide <= wide_row + lo, panel, 0.0)
            panels.append(panel)

        half = rank // 2

        def trail(first):
            for l in range(layers):
                work[l, first:, :] = jnp.where(own[first:, :], 0.0, work[l, first:, :]) - lax.dot_general(
                    panels[l][:, first:],
                    panels[l],
                    (((0,), (0,)), ((), ())),
                    precision=hi,
                    preferred_element_type=jnp.float32,
                )

        @pl.when(lo + block < half)
        def _():
            trail(0)

        @pl.when((lo + block >= half) & (lo + block < rank))
        def _():
            trail(half)

        return 0

    lax.fori_loop(0, rank // block, eliminate, 0)

def inverse_factor(gram):
    return pl.pallas_call(
        functools.partial(inverse_kernel, 32, 8),
        out_shape=jax.ShapeDtypeStruct(gram.shape, jnp.float32),
        in_specs=[pl.BlockSpec(memory_space=pltpu.VMEM)],
        out_specs=pl.BlockSpec(memory_space=pltpu.VMEM),
        scratch_shapes=[pltpu.VMEM(gram.shape, jnp.float32)],
        name="inverse_factor",
    )(gram)


def cross_kernel(part, here_ref, buffer_ref, power_ref, mine_ref, theirs_ref, whole):
    rest = power_ref[0]
    terms = []
    for _ in range(3):
        terms.append(rest.astype(jnp.bfloat16))
        rest = rest - terms[-1].astype(jnp.float32)
    total = lax.dot_general(
        buffer_ref[0],
        jnp.concatenate(terms, axis=1),
        (((0,), (0,)), ((), ())),
        preferred_element_type=jnp.float32,
    )
    rank = power_ref.shape[2]
    total = total[:, :rank] + (total[:, rank : 2 * rank] + total[:, 2 * rank :])
    padding = jnp.zeros((whole.shape[1] - part, whole.shape[2]), jnp.float32)
    for j in range(2 * Z_SIZE):
        whole[j] = jnp.concatenate([total[j * part : (j + 1) * part, :], padding], axis=0)
    z, core = here_ref[0], here_ref[1]
    for ref, owner in ((mine_ref, core), (theirs_ref, 1 - core)):
        for i in range(Z_SIZE):
            by = (1, 1, 3, 3, 2, 2, 4, 0)[i]
            place = lax.rem(z + by * (1 - 2 * owner) + Z_SIZE, Z_SIZE)
            whose = 1 - owner if i in (1, 3, 5) else owner
            ref[i, 0] = whole[2 * place + whose]


def cross(buffer16, power, padded):
    layers, rows, cols = buffer16.shape
    rank = power.shape[2]
    shape = jax.ShapeDtypeStruct((Z_SIZE, layers, padded, rank), jnp.float32)
    out_spec = pl.BlockSpec((Z_SIZE, 1, padded, rank), lambda l, here: (0, l, 0, 0))
    return pl.pallas_call(
        functools.partial(cross_kernel, cols // (2 * Z_SIZE)),
        out_shape=(shape, shape),
        grid_spec=pltpu.PrefetchScalarGridSpec(
            num_scalar_prefetch=1,
            grid=(layers,),
            in_specs=[
                pl.BlockSpec((1, rows, cols), lambda l, here: (l, 0, 0)),
                pl.BlockSpec((1, rows, rank), lambda l, here: (l, 0, 0)),
            ],
            out_specs=(out_spec, out_spec),
            scratch_shapes=[pltpu.VMEM((2 * Z_SIZE, padded, rank), jnp.float32)],
        ),
        cost_estimate=pl.CostEstimate(
            flops=6 * layers * rows * cols * rank,
            bytes_accessed=2 * layers * rows * cols + 16 * layers * Z_SIZE * padded * rank,
            transcendentals=0,
        ),
        name="cross",
    )(position(), buffer16, power)


def scatter_near(blocks):
    next_, four = lax.optimization_barrier((blocks[0:4], blocks[6]))
    next_, four = lax.optimization_barrier((turn(next_, 1), turn(four, 2)))
    two = jnp.stack([blocks[4] + next_[2] + four, blocks[5] + next_[3]])
    return blocks[7], next_[0:2], two


def scatter_end(own, one, far):
    total = one + far
    total = jnp.stack([own + total[0], total[1]])
    other = swap(total, CORE, 2, 1)
    return jnp.stack([total[0] + other[1], total[1] + other[0]])


def shards(grad, momentum, basis):
    hi = lax.Precision.HIGHEST
    scale = math.sqrt(D * FF / RANK)
    layers, rows, cols = grad.shape
    tp = lax.axis_index(TP)
    part = basis.shape[0]
    padded = -(-part // 16) * 16

    buffer = MOMENTUM_DECAY * momentum.astype(jnp.float32) + grad.astype(jnp.float32)
    shard = jnp.pad(basis.transpose(1, 0, 2), ((0, 0), (0, padded - part), (0, 0)))
    pieces, buffer16 = gather_both(shard, buffer.astype(jnp.bfloat16))
    partial = lax.all_to_all(power_step(buffer16, pieces, part), TP, 0, 0, tiled=True)
    power = lax.all_gather(partial.sum(0), TP, axis=1).reshape(layers, rows, RANK)

    share = RANK // TP_SIZE
    gram = jnp.einsum("lmr,lms->lrs", power, power, precision=hi)
    gram = lax.dynamic_slice_in_dim(gram, tp * share, share, 1)
    gram = gram + swap(gram, CORE, 2, 1)
    gram, right = lax.optimization_barrier((gram, power))
    mine, theirs = cross(buffer16, right, padded)
    theirs, gram = lax.optimization_barrier((theirs, add_one(gram)))
    gram = add_crossing(add_two(gram))
    mine = mine + swap(theirs, CORE, 2, 1)
    mine, gram = lax.optimization_barrier((mine, gram))
    hops = scatter_near(mine)

    gram = lax.all_gather(gram, TP, axis=1).reshape(layers, RANK, RANK)
    gram, hops = lax.optimization_barrier((gram, hops))
    own, one, two = hops
    far, inverse = lax.optimization_barrier((turn(two, 2), inverse_factor(gram)))
    mixed = scatter_end(own, one, far)
    project = jnp.einsum("clnr,lir->clni", mixed, inverse, precision=hi)
    colsq = jnp.sum(project * project, axis=2, keepdims=True)
    def ortho_step(total):
        ortho = jnp.einsum("lmr,lir->lmi", power, inverse, precision=hi).astype(jnp.bfloat16)
        return add_two(add_one(total)), ortho

    pieces, (colsq, ortho) = gather_fsdp(
        project.astype(jnp.bfloat16),
        colsq[0] + colsq[1],
        lambda total: add_four(Y, add_four(X, total)),
        ortho_step,
        lambda side: (add_crossing(side[0]), side[1]),
    )
    norm = lax.rsqrt(colsq + EPSILON)
    basis_next = (project[0, :, :part] * norm).astype(jnp.bfloat16).transpose(1, 0, 2)
    momentum_next, update = finish(grad, momentum, ortho, norm, pieces, part, scale)
    return (momentum_next, basis_next, update)


def solution(mesh):
    torus = Mesh(mesh.devices.reshape(8, 2, 4, 4), FSDP + TP)
    return jax.shard_map(
        shards,
        mesh=torus,
        in_specs=(P(None, FSDP, TP), P(None, FSDP, TP), P(TP_FSDP, None, None)),
        out_specs=(P(None, FSDP, TP), P(TP_FSDP, None, None), P(None, FSDP, TP)),
        check_vma=False,
    )
```

```python
import functools
import math

import jax
import jax.numpy as jnp
from jax import lax
from jax.experimental import pallas as pl
from jax.experimental.pallas import tpu as pltpu
from jax.sharding import Mesh
from jax.sharding import PartitionSpec as P

D = 5120
FF = 27648
RANK = 256
LAYERS = 3
Z, CORE, X, Y = "fsdp_0", "fsdp_1", "tp_0", "tp_1"
FSDP = (Z, CORE)
TP = (X, Y)
TP_FSDP = TP + FSDP
Z_SIZE = 8
TP_SIZE = 16

MOMENTUM_DECAY = 0.8
EPSILON = 1e-06


def shift(value, axis, size, by):
    return lax.ppermute(value, axis, [(i, (i + by) % size) for i in range(size)])


def swap(value, axis, size, bit):
    return lax.ppermute(value, axis, [(i, i ^ bit) for i in range(size)])


def turn(value, by):
    pairs = []
    for z in range(Z_SIZE):
        pairs.append((2 * z, 2 * ((z + by) % Z_SIZE)))
        pairs.append((2 * z + 1, 2 * ((z - by) % Z_SIZE) + 1))
    return lax.ppermute(value, FSDP, pairs)


def position():
    return jnp.stack([lax.axis_index(Z), lax.axis_index(CORE)]).astype(jnp.int32)


def crossing(value):
    pairs = []
    for z in range(Z_SIZE):
        pairs.append((2 * z, 2 * ((z + 1) % Z_SIZE) + 1))
        pairs.append((2 * z + 1, 2 * ((z - 1) % Z_SIZE)))
    return lax.ppermute(value, FSDP, pairs)


def spin(value, axis, by, cores=0):
    pairs = []
    for i in range(4):
        pairs.append((i, (i + by) % 4 + 4 * cores))
        pairs.append((4 + i, (i - by) % 4 + 4 * (1 - cores)))
    return lax.ppermute(value, (CORE, axis), pairs)


def add_one(value):
    return value + turn(value, 1)


def add_two(value):
    return value + turn(value, 2)


def add_crossing(value):
    return value + crossing(value)


def add_four(axis, value):
    value = value + spin(value, axis, 1)
    return value + spin(value, axis, 1, 1)


RING_SEATS = (
    tuple((0, 0, i) for i in (0, 1)),
    tuple((0, 1 + i // 2, i % 2) for i in range(4)),
    tuple((0, -1 - i // 2, 1 - i % 2) for i in range(4)),
    tuple((0, 3 + i // 2, i % 2) for i in range(3)),
    tuple((0, -3 - i // 2, 1 - i % 2) for i in range(3)),
)
BOTH_SEATS = tuple(
    tuple((by, 0, other) for by in group)
    for group in ((0, 7, 1, 6, 2), (5, 3, 4))
    for other in (0, 1)
)


def gather_both(shard, busy):
    half = shard.shape[2] // 2
    left, right = shift(shard, Z, Z_SIZE, 1), shift(shard, Z, Z_SIZE, -1)
    left2, right2 = shift(shard, Z, Z_SIZE, 2), shift(shard, Z, Z_SIZE, -2)
    left3, right3 = shift(left2, Z, Z_SIZE, 1), shift(right2, Z, Z_SIZE, -1)
    far_left = shift(left2[:, :, :half], Z, Z_SIZE, 2)
    far_right = shift(right2[:, :, half:], Z, Z_SIZE, -2)
    left3, right3, far_left, far_right, busy = lax.optimization_barrier(
        (left3, right3, far_left, far_right, busy)
    )
    near = jnp.stack([shard, left, right, left2, right2])
    near2 = swap(near, CORE, 2, 1)
    far = jnp.stack([left3, right3, jnp.concatenate([far_left, far_right], axis=2)])
    far2 = swap(far, CORE, 2, 1)
    return (near, near2, far, far2), busy


def gather_fsdp(pair, side, first, second, last):
    one, two, side = lax.optimization_barrier((turn(pair, 1), turn(pair, 2), first(side)))
    three, four = turn(two, 1), turn(two[0], 2)
    near = jnp.concatenate([one, two])
    near2 = swap(near, CORE, 2, 1)
    three, four, side = lax.optimization_barrier((three, four, second(side)))
    far = jnp.concatenate([three, four[None]])
    far2 = swap(far, CORE, 2, 1)
    return (pair, near, near2, far, far2), last(side)


def join(rows, seats, here_ref, refs, layer, blocks):
    z, core = here_ref[0], here_ref[1]
    ahead = 2 * core - 1
    for ref, group in zip(refs, seats):
        for i, (by, way, other) in enumerate(group):
            place = lax.rem(z + by + way * ahead + Z_SIZE, Z_SIZE)
            whose = 1 - core if other else core
            blocks[2 * place + whose] = ref[i, layer].astype(jnp.float32)
    return jnp.concatenate([blocks[j][:rows, :] for j in range(2 * Z_SIZE)], axis=0)


def finish_kernel(rows, scale, here_ref, grad_ref, momentum_ref, ortho_ref, norm_ref, *refs):
    momentum_next_ref, update_ref, blocks = refs[-3:]
    whole = join(rows, RING_SEATS, here_ref, refs[:-3], 0, blocks).astype(jnp.bfloat16)
    ortho = ortho_ref[0]
    scaled = (ortho.astype(jnp.float32) * (scale * norm_ref[0])).astype(jnp.bfloat16)
    both = lax.dot_general(
        jnp.concatenate([ortho, scaled], axis=0),
        whole,
        (((1,), (1,)), ((), ())),
        preferred_element_type=jnp.float32,
    )
    height = ortho.shape[0]
    feedback, update = both[:height, :], both[height:, :]
    buffer = MOMENTUM_DECAY * momentum_ref[0].astype(jnp.float32) + grad_ref[0].astype(jnp.float32)
    momentum_next_ref[0] = (buffer - (1.0 - MOMENTUM_DECAY) * feedback).astype(jnp.bfloat16)
    update_ref[0] = update.astype(jnp.bfloat16)


def power_kernel(rows, here_ref, buffer_ref, *refs):
    out_ref, blocks = refs[-2:]
    whole = join(rows, BOTH_SEATS, here_ref, refs[:-2], 0, blocks).astype(jnp.bfloat16)
    product = jnp.dot(buffer_ref[0], whole, preferred_element_type=jnp.float32)
    share = out_ref.shape[2]
    for t in range(out_ref.shape[0]):
        out_ref[t, 0] = product[t * share : (t + 1) * share, :]


def piece_specs(pieces):
    return [
        pl.BlockSpec((p.shape[0], 1) + p.shape[2:], lambda *ids: (0, ids[0], 0, 0)) for p in pieces
    ]


def finish(grad, momentum, ortho, norm, pieces, rows, scale):
    layers, height, cols = grad.shape
    padded, rank = pieces[0].shape[2:]
    shape = jax.ShapeDtypeStruct(grad.shape, grad.dtype)

    def spec(m, n):
        return pl.BlockSpec((1, m, n), lambda l, here: (l, 0, 0))

    return pl.pallas_call(
        functools.partial(finish_kernel, rows, scale),
        out_shape=(shape, shape),
        grid_spec=pltpu.PrefetchScalarGridSpec(
            num_scalar_prefetch=1,
            grid=(layers,),
            in_specs=[spec(height, cols), spec(height, cols), spec(height, rank), spec(1, rank)]
            + piece_specs(pieces),
            out_specs=(spec(height, cols), spec(height, cols)),
            scratch_shapes=[pltpu.VMEM((2 * Z_SIZE, padded, rank), jnp.float32)],
        ),
        name="finish",
    )(position(), grad, momentum, ortho, norm, *pieces)


def power_step(buffer16, pieces, rows):
    layers, height, cols = buffer16.shape
    padded, rank = pieces[0].shape[2:]
    share = height // TP_SIZE
    return pl.pallas_call(
        functools.partial(power_kernel, rows),
        out_shape=jax.ShapeDtypeStruct((TP_SIZE, layers, share, rank), jnp.float32),
        grid_spec=pltpu.PrefetchScalarGridSpec(
            num_scalar_prefetch=1,
            grid=(layers,),
            in_specs=[pl.BlockSpec((1, height, cols), lambda l, here: (l, 0, 0))]
            + piece_specs(pieces),
            out_specs=pl.BlockSpec((TP_SIZE, 1, share, rank), lambda l, here: (0, l, 0, 0)),
            scratch_shapes=[pltpu.VMEM((2 * Z_SIZE, padded, rank), jnp.float32)],
        ),
        name="power",
    )(position(), buffer16, *pieces)


def inverse_kernel(block, group, gram_ref, out_ref, work):
    layers, rank = gram_ref.shape[0], gram_ref.shape[1]
    hi = lax.Precision.HIGHEST
    row = lax.broadcasted_iota(jnp.int32, (block, block), 0)
    lane = lax.broadcasted_iota(jnp.int32, (block, block), 1)
    eye = (row == lane).astype(jnp.float32)
    row_id = lax.broadcasted_iota(jnp.int32, (block, 2 * block), 0)
    wide = lax.broadcasted_iota(jnp.int32, (block, rank), 1)
    wide_row = lax.broadcasted_iota(jnp.int32, (block, rank), 0)
    place = lax.broadcasted_iota(jnp.int32, (rank, rank), 1)
    work[...] = gram_ref[...]

    def eliminate(step, _):
        lo = pl.multiple_of(step * block, block)
        tops = [work[l, pl.ds(lo, block), :] for l in range(layers)]
        diag = [pltpu.roll(top, rank - lo, 1)[:, :block] for top in tops]
        tails = [jnp.concatenate([d, eye], axis=1) for d in diag]
        ready = [[] for _ in range(layers)]
        for first in range(0, block, group):
            cols = [
                [jnp.broadcast_to(tail[:, c : c + 1], tail.shape) for c in range(first, first + group)]
                for tail in tails
            ]
            below = row_id[first:, :]
            for j in range(group):
                for l in range(layers):
                    tail, col = tails[l], cols[l]
                    factor = jnp.where(below > first + j, col[j] * (1.0 / col[j][j : j + 1, :]), 0.0)
                    for later in range(j + 1, group):
                        col[later] = col[later] - factor * col[later][j : j + 1, :]
                    tails[l] = tail - factor * tail[j : j + 1, :]
            for l in range(layers):
                ready[l].append(tails[l][:group, :])
                tails[l] = tails[l][group:, :]
        mats = [jnp.concatenate(parts, axis=0) for parts in ready]
        inside = (wide >= lo) & (wide < lo + block)
        unit = (wide - lo == wide_row).astype(jnp.float32)
        panels = []
        own = (place >= lo) & (place < lo + block)
        for l in range(layers):
            mat = mats[l]
            pivots = jnp.sum(jnp.where(row == lane, mat[:, :block], 0.0), axis=1, keepdims=True)
            small = mat[:, block:] * lax.rsqrt(pivots)
            panel = jnp.dot(small, jnp.where(inside, unit, tops[l]), precision=hi, preferred_element_type=jnp.float32)
            out_ref[l, pl.ds(lo, block), :] = jnp.where(wide <= wide_row + lo, panel, 0.0)
            panels.append(panel)

        half = rank // 2

        def trail(first):
            for l in range(layers):
                work[l, first:, :] = jnp.where(own[first:, :], 0.0, work[l, first:, :]) - lax.dot_general(
                    panels[l][:, first:],
                    panels[l],
                    (((0,), (0,)), ((), ())),
                    precision=hi,
                    preferred_element_type=jnp.float32,
                )

        @pl.when(lo + block < half)
        def _():
            trail(0)

        @pl.when((lo + block >= half) & (lo + block < rank))
        def _():
            trail(half)

        return 0

    lax.fori_loop(0, rank // block, eliminate, 0)

def inverse_factor(gram):
    return pl.pallas_call(
        functools.partial(inverse_kernel, 32, 8),
        out_shape=jax.ShapeDtypeStruct(gram.shape, jnp.float32),
        in_specs=[pl.BlockSpec(memory_space=pltpu.VMEM)],
        out_specs=pl.BlockSpec(memory_space=pltpu.VMEM),
        scratch_shapes=[pltpu.VMEM(gram.shape, jnp.float32)],
        name="inverse_factor",
    )(gram)


def cross_kernel(part, here_ref, buffer_ref, power_ref, mine_ref, theirs_ref, whole):
    rest = power_ref[0]
    terms = []
    for _ in range(3):
        terms.append(rest.astype(jnp.bfloat16))
        rest = rest - terms[-1].astype(jnp.float32)
    total = lax.dot_general(
        buffer_ref[0],
        jnp.concatenate(terms, axis=1),
        (((0,), (0,)), ((), ())),
        preferred_element_type=jnp.float32,
    )
    rank = power_ref.shape[2]
    total = total[:, :rank] + (total[:, rank : 2 * rank] + total[:, 2 * rank :])
    padding = jnp.zeros((whole.shape[1] - part, whole.shape[2]), jnp.float32)
    for j in range(2 * Z_SIZE):
        whole[j] = jnp.concatenate([total[j * part : (j + 1) * part, :], padding], axis=0)
    z, core = here_ref[0], here_ref[1]
    for ref, owner in ((mine_ref, core), (theirs_ref, 1 - core)):
        for i in range(Z_SIZE):
            by = (1, 1, 3, 3, 2, 2, 4, 0)[i]
            place = lax.rem(z + by * (1 - 2 * owner) + Z_SIZE, Z_SIZE)
            whose = 1 - owner if i in (1, 3, 5) else owner
            ref[i, 0] = whole[2 * place + whose]


def cross(buffer16, power, padded):
    layers, rows, cols = buffer16.shape
    rank = power.shape[2]
    shape = jax.ShapeDtypeStruct((Z_SIZE, layers, padded, rank), jnp.float32)
    out_spec = pl.BlockSpec((Z_SIZE, 1, padded, rank), lambda l, here: (0, l, 0, 0))
    return pl.pallas_call(
        functools.partial(cross_kernel, cols // (2 * Z_SIZE)),
        out_shape=(shape, shape),
        grid_spec=pltpu.PrefetchScalarGridSpec(
            num_scalar_prefetch=1,
            grid=(layers,),
            in_specs=[
                pl.BlockSpec((1, rows, cols), lambda l, here: (l, 0, 0)),
                pl.BlockSpec((1, rows, rank), lambda l, here: (l, 0, 0)),
            ],
            out_specs=(out_spec, out_spec),
            scratch_shapes=[pltpu.VMEM((2 * Z_SIZE, padded, rank), jnp.float32)],
        ),
        cost_estimate=pl.CostEstimate(
            flops=6 * layers * rows * cols * rank,
            bytes_accessed=2 * layers * rows * cols + 16 * layers * Z_SIZE * padded * rank,
            transcendentals=0,
        ),
        name="cross",
    )(position(), buffer16, power)


def scatter_near(blocks):
    next_, four = lax.optimization_barrier((blocks[0:4], blocks[6]))
    next_, four = lax.optimization_barrier((turn(next_, 1), turn(four, 2)))
    two = jnp.stack([blocks[4] + next_[2] + four, blocks[5] + next_[3]])
    return blocks[7], next_[0:2], two


def scatter_end(own, one, far):
    total = one + far
    total = jnp.stack([own + total[0], total[1]])
    other = swap(total, CORE, 2, 1)
    return jnp.stack([total[0] + other[1], total[1] + other[0]])


def shards(grad, momentum, basis):
    hi = lax.Precision.HIGHEST
    scale = math.sqrt(D * FF / RANK)
    layers, rows, cols = grad.shape
    tp = lax.axis_index(TP)
    part = basis.shape[0]
    padded = -(-part // 16) * 16

    buffer = MOMENTUM_DECAY * momentum.astype(jnp.float32) + grad.astype(jnp.float32)
    shard = jnp.pad(basis.transpose(1, 0, 2), ((0, 0), (0, padded - part), (0, 0)))
    pieces, buffer16 = gather_both(shard, buffer.astype(jnp.bfloat16))
    partial = lax.all_to_all(power_step(buffer16, pieces, part), TP, 0, 0, tiled=True)
    power = lax.all_gather(partial.sum(0), TP, axis=1).reshape(layers, rows, RANK)

    share = RANK // TP_SIZE
    gram = jnp.einsum("lmr,lms->lrs", power, power, precision=hi)
    gram = lax.dynamic_slice_in_dim(gram, tp * share, share, 1)
    gram = gram + swap(gram, CORE, 2, 1)
    gram, right = lax.optimization_barrier((gram, power))
    mine, theirs = cross(buffer16, right, padded)
    theirs, gram = lax.optimization_barrier((theirs, add_one(gram)))
    gram = add_crossing(add_two(gram))
    mine = mine + swap(theirs, CORE, 2, 1)
    mine, gram = lax.optimization_barrier((mine, gram))
    hops = scatter_near(mine)

    gram = lax.all_gather(gram, TP, axis=1).reshape(layers, RANK, RANK)
    gram, hops = lax.optimization_barrier((gram, hops))
    own, one, two = hops
    far, inverse = lax.optimization_barrier((turn(two, 2), inverse_factor(gram)))
    mixed = scatter_end(own, one, far)
    project = jnp.einsum("clnr,lir->clni", mixed, inverse, precision=hi)
    colsq = jnp.sum(project * project, axis=2, keepdims=True)
    def ortho_step(total):
        ortho = jnp.einsum("lmr,lir->lmi", power, inverse, precision=hi).astype(jnp.bfloat16)
        return total + turn(total, 1) + turn(total, 2) + turn(total, 3), ortho

    pieces, (colsq, ortho) = gather_fsdp(
        project.astype(jnp.bfloat16),
        colsq[0] + colsq[1],
        lambda total: add_four(Y, add_four(X, total)),
        ortho_step,
        lambda side: (add_crossing(side[0]), side[1]),
    )
    norm = lax.rsqrt(colsq + EPSILON)
    basis_next = (project[0, :, :part] * norm).astype(jnp.bfloat16).transpose(1, 0, 2)
    momentum_next, update = finish(grad, momentum, ortho, norm, pieces, part, scale)
    return (momentum_next, basis_next, update)


def solution(mesh):
    torus = Mesh(mesh.devices.reshape(8, 2, 4, 4), FSDP + TP)
    return jax.shard_map(
        shards,
        mesh=torus,
        in_specs=(P(None, FSDP, TP), P(None, FSDP, TP), P(TP_FSDP, None, None)),
        out_specs=(P(None, FSDP, TP), P(TP_FSDP, None, None), P(None, FSDP, TP)),
        check_vma=False,
    )
```
